32 devices in a mesh: grp: 2 (over y), ctx: 4 (over z), sub: 4 (over x, core).
Axes of the slice: x: 2, y: 2, z: 4, core: 2. Of those that a mesh axis runs over, the one named last changes fastest.
Arguments:
- queries: bfloat16 [64, 3072], P(('grp', 'ctx'), 'sub'), parts along dimension 0, may hold values from -1024 to 1024
- latent_cache: bfloat16 [3072, 576], P(('grp', 'ctx')), parts along dimension 0, may hold values from -8 to 8
- cache_len: int32 [8], P(('grp', 'ctx')), parts along dimension 0, may hold values from 16 to 384, as said below
- kv_up: bfloat16 [32, 256, 512], P(('grp', 'sub'), None, 'ctx'), parts along dimension 0, may hold values from -1 to 1
- o_weight: bfloat16 [2048, 2048], P('sub', 'ctx'), may hold values from -0.5 to 0.5
- residual: bfloat16 [64, 2048], P(('grp', 'ctx')), parts along dimension 0, may hold values from -3 to 3
- norm_gain: bfloat16 [2048], replicated, may hold values from 0.25 to 1.75
- route_ids: int32 [64, 6], P(('grp', 'ctx')), parts along dimension 0, may hold values from 0 to 63, all different within a row; in each aligned block of 8 rows (0 to 7, 8 to 15, ...) at most 2 rows name the same one
- route_weights: float32 [64, 6], P(('grp', 'ctx')), parts along dimension 0, may hold values from 0.1 to 0.6
- w_gate: bfloat16 [64, 2048, 1408], P('ctx', None, 'sub'), may hold values from -0.125 to 0.125
- w_up: bfloat16 [64, 2048, 1408], P('ctx', None, 'sub'), may hold values from -0.125 to 0.125
- w_down: bfloat16 [64, 1408, 2048], P('ctx', 'sub'), may hold values from -0.15625 to 0.15625
Outputs:
- layer_out: bfloat16 [64, 2048], P(('grp', 'ctx'), 'sub'), parts along dimension 0
The draws below stay inside these ranges and needn't reach their ends.
There are 2 independent parts, one for each index of `grp`. The reference program is written for one: setup_inputs(seed, part) draws one part's arguments, and reference() takes and returns one part's arrays. A program takes and returns all parts, laid end to end along the dimension named above; an argument that names none is the same for every part. Nothing has to cross between parts.
Inputs may be any that keep to these rules, and one draw needn't show every extreme that they name: `route_ids`: each row names 6 different experts. Among the 8 rows of one ctx index no expert is named more than 2 times, and in every draw some expert is named exactly 2 times by the rows of some ctx index. cache_len[c] positions at the start of shard c are live; at least one shard is full.
All inputs are finite; a program needn't handle non-finite values.
Results may differ from the reference program's by a relative error of at most 0.015.
Values may be sent and summed in bfloat16 or wider, within the bound.
A program may use at most 128 MiB of HBM per device.

```python
import math
import jax
import jax.numpy as jnp
import numpy as np
from jax import lax

D = 2048
HEADS = 16
NOPE = 128
ROPE = 64
VDIM = 128
LATENT = 512
FF = 1408
EXPERTS = 64
TOP = 6
TOK_DEV = 8
CACHE_DEV = 384
CAP = 2
SPAN = 32
CACHE = 1536
N_CTX = 4


def draw_tables(key):
    base_key = jax.random.fold_in(key, 7)
    cache_key, up_key, query_key = jax.random.split(base_key, 3)
    row_width = LATENT + ROPE
    cache_rows = jnp.clip(jax.random.normal(cache_key, (CACHE, row_width), jnp.float32), -6.0, 6.0)
    up_table = jnp.clip(jax.random.normal(up_key, (HEADS, NOPE + VDIM, LATENT), jnp.float32), -6.0, 6.0) * LATENT ** (-0.5)
    query_table = jnp.clip(jax.random.normal(query_key, (SPAN, HEADS, NOPE + ROPE), jnp.float32), -6.0, 6.0) * 2.5
    return (cache_rows, up_table, query_table)


def draw_queries(key, part):
    tables = draw_tables(key)
    return tables[2].reshape(SPAN, HEADS * (NOPE + ROPE)).astype(jnp.bfloat16)


def draw_latent_cache(key, part):
    tables = draw_tables(key)
    return tables[0].astype(jnp.bfloat16)


def draw_kv_up(key, part):
    tables = draw_tables(key)
    return tables[1].astype(jnp.bfloat16)


def draw_cache_len(key, part):
    length_key, full_key = jax.random.split(jax.random.fold_in(key, 11))
    halvings = jax.random.randint(length_key, (N_CTX,), 0, 5)
    lengths = jnp.maximum(jnp.right_shift(jnp.full((N_CTX,), CACHE_DEV, jnp.int32), halvings.astype(jnp.int32)), 16)
    full_index = jax.random.randint(full_key, (), 0, N_CTX)
    return jnp.where(jnp.arange(N_CTX, dtype=jnp.int32) == full_index, CACHE_DEV, lengths).astype(jnp.int32)


def shard_levels(key, dims, cuts, least, top_value):
    def one(position, blocks):
        draws = jax.random.uniform(jax.random.fold_in(jax.random.fold_in(key, 6), position), (blocks,), jnp.float32, least / len(cuts), top_value / len(cuts))
        return jnp.repeat(jnp.exp(draws), dims[position] // blocks).reshape((-1,) + (1,) * (len(dims) - position - 1))

    gain = one(*cuts[0])
    for cut in cuts[1:]:
        gain = gain * one(*cut)
    return gain


def assign_block(rng, own, number, rows, count, top, bound, lean):
    ranking = jax.random.permutation(rng, count)
    packed, usual = portions_of(count, rows * top, bound, lean, True), portions_of(count, rows * top, bound, lean, False)
    places = jnp.arange(count)

    def named(sizes, rotation):
        used = int((sizes > 0).sum())
        fixed = max(1, used // 4)
        moved = fixed + (places - fixed + rotation * (used - fixed)) % max(1, count - fixed)
        return jnp.zeros((count,), jnp.int32).at[ranking[jnp.where(places < fixed, places, moved)]].set(jnp.asarray(sizes, jnp.int32))

    sizes = jnp.where(number % 4 == 0, named(packed, number // 4), named(usual, number - number // 4 - 1))
    mixed = jax.random.permutation(jax.random.fold_in(own, 3), count)
    giver, sink = mixed[0:count // 2 * 2:2], mixed[1:count // 2 * 2:2]
    margin = jnp.minimum(sizes[giver] - 1, bound - sizes[sink]) // 2
    margin = jnp.where((giver == ranking[0]) | (sink == ranking[0]) | (sizes[sink] == 0), 0, jnp.maximum(margin, 0))
    moved = jax.random.randint(jax.random.fold_in(own, 4), (count // 2,), 0, 1 << 20) % (margin + 1)
    sizes = sizes.at[giver].add(-moved).at[sink].add(moved)
    items = jnp.searchsorted(jnp.cumsum(sizes), jnp.arange(rows * top), side="right").astype(jnp.int32)
    table = items.reshape(top, rows).T
    table = table[jax.random.permutation(jax.random.fold_in(own, 1), rows)]
    rotation = jax.random.randint(jax.random.fold_in(own, 2), (rows, 1), 0, top)
    return jnp.take_along_axis(table, (jnp.arange(top)[None, :] + rotation) % top, axis=1)


def portions_of(number_of, total, bound, lean, full):
    loads = [(1 << 20) // math.isqrt(standing ** lean) + 1 for standing in range(1, number_of + 1)]
    largest = bound if full else min(bound, max(-(-total // number_of), total * loads[0] // sum(loads)))
    least = 1 if total - largest >= number_of - 1 else 0
    counts, spare = [largest] + [least] * (number_of - 1), total - largest - least * (number_of - 1)
    while spare > 0:
        movable = [i for i in range(1, number_of) if counts[i] < largest] or [i for i in range(1, number_of) if counts[i] < bound]
        pool, budget = sum([loads[i] for i in movable]), spare
        for i in movable:
            extra = min(bound - counts[i], max(1, budget * loads[i] // pool), spare)
            counts[i] = counts[i] + extra
            spare = spare - extra
    return np.array(counts)


def bell_draw(key, extent, spread, reach, cuts=(), kind=jnp.bfloat16):
    loudness = shard_levels(key, extent, cuts, -0.22, 0.18) if cuts else 1.0
    array = jax.random.normal(key, extent, jnp.float32) * spread * loudness
    return jnp.minimum(jnp.maximum(array, -reach), reach).astype(kind)


def setup_inputs(seed: int = 0, part: int = 0) -> dict:
    keys = jax.random.split(jax.random.key(seed), 13)
    part_keys = jax.random.split(jax.random.fold_in(keys[12], part), 13)
    queries = draw_queries(jax.random.fold_in(jax.random.fold_in(keys[12], part), 71), part)
    latent_cache = draw_latent_cache(jax.random.fold_in(jax.random.fold_in(keys[12], part), 71), part)
    cache_len = draw_cache_len(jax.random.fold_in(jax.random.fold_in(keys[12], part), 71), part)
    kv_up = draw_kv_up(jax.random.fold_in(jax.random.fold_in(keys[12], part), 71), part)
    o_weight = bell_draw(keys[4], (HEADS * VDIM, D), (HEADS * VDIM // 16) ** -0.5, 0.5, ((0, 4), (1, 4)))
    residual = bell_draw(part_keys[5], (SPAN, D), 0.5, 3.0, ((0, 4),))
    norm_gain = jnp.clip(1.0 + 0.15 * jax.random.normal(keys[6], (D,), jnp.float32), 0.25, 1.75).astype(jnp.bfloat16)
    route_ids_keys = jax.random.split(jax.random.fold_in(part_keys[7], 1), SPAN // TOK_DEV)
    route_ids_turns = jax.random.permutation(jax.random.fold_in(part_keys[7], 3), SPAN // TOK_DEV)
    route_ids = jax.vmap(lambda own, number: assign_block(jax.random.fold_in(part_keys[7], 2), own, number, TOK_DEV, EXPERTS, TOP, CAP, 2))(route_ids_keys, route_ids_turns).reshape((SPAN, TOP))
    route_weights = jnp.clip(0.1 + 0.5 * jax.random.uniform(part_keys[8], (SPAN, TOP), jnp.float32) ** shard_levels(part_keys[8], (SPAN, TOP), ((0, 4),), -0.2, 0.2), 0.1, 0.6)
    w_gate = bell_draw(keys[9], (EXPERTS, D, FF), D ** -0.5, 0.125, ((0, 4), (2, 4)))
    w_up = bell_draw(keys[10], (EXPERTS, D, FF), D ** -0.5, 0.125, ((0, 4), (2, 4)))
    w_down = bell_draw(keys[11], (EXPERTS, FF, D), FF ** -0.5, 0.15625, ((0, 4), (1, 4)))
    return dict(queries=queries, latent_cache=latent_cache, cache_len=cache_len, kv_up=kv_up, o_weight=o_weight, residual=residual, norm_gain=norm_gain, route_ids=route_ids, route_weights=route_weights, w_gate=w_gate, w_up=w_up, w_down=w_down)


epsilon = 1e-06

def shard_attention(absorbed, cache_rows, live_mask, up_value):
    scores = jnp.einsum('qhc,kc->qhk', absorbed.astype(jnp.float32), cache_rows.astype(jnp.float32)) * (NOPE + ROPE) ** (-0.5)
    scores = jnp.where(live_mask[None, None, :], scores, -jnp.inf)
    highest = lax.optimization_barrier(jnp.max(scores, axis=2))
    weights = jnp.exp(scores - highest[:, :, None]).astype(jnp.bfloat16)
    totals = lax.optimization_barrier(jnp.sum(weights.astype(jnp.float32), axis=2))
    latent_out = jnp.einsum('qhk,kl->qhl', weights.astype(jnp.float32), cache_rows[:, :LATENT].astype(jnp.float32)).astype(jnp.bfloat16)
    head_out = jnp.einsum('qhl,hvl->qhv', latent_out.astype(jnp.float32), up_value.astype(jnp.float32))
    return (highest, totals, head_out)

def reference(queries, latent_cache, cache_len, kv_up, o_weight, residual, norm_gain, route_ids, route_weights, w_gate, w_up, w_down):
    query_heads = queries.reshape(SPAN, HEADS, NOPE + ROPE)
    query_latent = jnp.einsum('qhn,hnl->qhl', query_heads[:, :, :NOPE].astype(jnp.float32), kv_up[:, :NOPE, :].astype(jnp.float32)).astype(jnp.bfloat16)
    absorbed = jnp.concatenate([query_latent, query_heads[:, :, NOPE:]], axis=2)
    up_value = kv_up[:, NOPE:, :]
    blocks = latent_cache.reshape(N_CTX, CACHE_DEV, LATENT + ROPE)
    positions = jnp.arange(CACHE_DEV, dtype=jnp.int32)

    def fold_shard(running, shard_item):
        highest, totals, summed = running
        cache_rows, length = shard_item
        shard_high, shard_total, shard_head = shard_attention(absorbed, cache_rows, positions < length, up_value)
        new_high = jnp.maximum(highest, shard_high)
        old_factor = jnp.exp(highest - new_high)
        new_factor = jnp.exp(shard_high - new_high)
        return ((new_high, totals * old_factor + shard_total * new_factor, summed * old_factor[:, :, None] + shard_head * new_factor[:, :, None]), None)
    initial = (jnp.full((SPAN, HEADS), -jnp.inf, jnp.float32), jnp.zeros((SPAN, HEADS), jnp.float32), jnp.zeros((SPAN, HEADS, VDIM), jnp.float32))
    (highest, totals, summed), unused = lax.scan(fold_shard, initial, (blocks, cache_len))
    attention = (summed / totals[:, :, None]).astype(jnp.bfloat16).reshape(SPAN, HEADS * VDIM)
    hidden = residual.astype(jnp.float32) + jnp.dot(attention, o_weight, preferred_element_type=jnp.float32)
    inverse_rms = lax.rsqrt(lax.optimization_barrier(jnp.mean(hidden * hidden, axis=1)) + epsilon)
    normed = (hidden * inverse_rms[:, None] * norm_gain.astype(jnp.float32)).astype(jnp.bfloat16)
    pair_count = TOK_DEV * TOP
    expert_ids = route_ids.reshape(N_CTX, pair_count)
    onehot = (expert_ids[:, :, None] == jnp.arange(EXPERTS, dtype=jnp.int32)[None, None, :]).astype(jnp.int32)
    earlier = jnp.cumsum(onehot, axis=1) - onehot
    slot_ids = lax.optimization_barrier(jnp.sum(earlier * onehot, axis=2))
    targets = (expert_ids * CAP + slot_ids).reshape(N_CTX, TOK_DEV, TOP)
    columns = jnp.arange(EXPERTS * CAP, dtype=jnp.int32)
    matches = targets[:, :, :, None] == columns[None, None, None, :]
    select = lax.optimization_barrier(jnp.sum(matches.astype(jnp.float32), axis=2))
    normed_blocks = normed.reshape(N_CTX, TOK_DEV, D)
    dispatched = jnp.einsum('ctj,ctd->cjd', select, normed_blocks.astype(jnp.float32)).astype(jnp.bfloat16)
    by_expert = dispatched.reshape(N_CTX, EXPERTS, CAP, D).transpose(1, 0, 2, 3).reshape(EXPERTS, N_CTX * CAP, D)

    def run_expert(operands):
        rows_in, gate_matrix, up_matrix, down_matrix = operands
        gate_act = jnp.dot(rows_in, gate_matrix, preferred_element_type=jnp.float32)
        up_act = jnp.dot(rows_in, up_matrix, preferred_element_type=jnp.float32)
        gated_rows = (jax.nn.silu(gate_act) * up_act).astype(jnp.bfloat16)
        return jnp.dot(gated_rows, down_matrix, preferred_element_type=jnp.float32).astype(jnp.bfloat16)
    expert_out = lax.map(run_expert, (by_expert, w_gate, w_up, w_down))
    back_rows = expert_out.reshape(EXPERTS, N_CTX, CAP, D).transpose(1, 0, 2, 3).reshape(N_CTX, EXPERTS * CAP, D)
    mixing = lax.optimization_barrier(jnp.sum(jnp.where(matches, route_weights.reshape(N_CTX, TOK_DEV, TOP)[:, :, :, None], 0.0), axis=2))
    routed = jnp.einsum('ctj,cjd->ctd', mixing, back_rows.astype(jnp.float32), precision=lax.Precision.HIGHEST)
    return (hidden + routed.reshape(SPAN, D)).astype(jnp.bfloat16)
```

```python
import functools

import jax
import jax.numpy as jnp
from jax import lax
from jax.experimental import pallas as pl
from jax.experimental.pallas import tpu as pltpu
from jax.sharding import PartitionSpec as P

D = 2048
NOPE = 128
ROPE = 64
VDIM = 128
LATENT = 512
TOP = 6
CAP = 2


epsilon = 1e-06


def local_attention(absorbed, cache_rows, length, up_value):
    scores = jnp.einsum("qhc,kc->qhk", absorbed, cache_rows, preferred_element_type=jnp.float32) * (
        NOPE + ROPE
    ) ** (-0.5)
    live_mask = lax.broadcasted_iota(jnp.int32, (cache_rows.shape[0],), 0) < length
    scores = jnp.where(live_mask[None, None, :], scores, -jnp.inf)
    highest = jnp.max(scores, axis=2)
    weights = jnp.exp(scores - highest[:, :, None]).astype(jnp.bfloat16)
    totals = jnp.sum(weights, axis=2, dtype=jnp.float32)
    latent_out = jnp.einsum(
        "qhk,kl->qhl", weights, cache_rows[:, :LATENT], preferred_element_type=jnp.float32
    ).astype(jnp.bfloat16)
    head_out = jnp.einsum("qhl,hvl->qhv", latent_out, up_value, preferred_element_type=jnp.float32)
    return (highest, totals, head_out)


def body(
    queries,
    latent_cache,
    cache_len,
    kv_up,
    o_weight,
    residual,
    norm_gain,
    route_ids,
    route_weights,
    w_gate,
    w_up,
    w_down,
):
    ctx_count = lax.axis_size("ctx")
    sub_count = lax.axis_size("sub")
    heads_dev = kv_up.shape[0]
    token_count = queries.shape[0]
    up_full = lax.all_gather(kv_up, "ctx", axis=2, tiled=True)
    up_key = up_full[:, :NOPE, :]
    up_value = up_full[:, NOPE:, :]
    own_rows = queries.reshape(token_count, heads_dev, NOPE + ROPE)
    query_latent = jnp.einsum(
        "qhn,hnl->qhl", own_rows[:, :, :NOPE], up_key, preferred_element_type=jnp.float32
    ).astype(jnp.bfloat16)
    mine = jnp.concatenate([query_latent, own_rows[:, :, NOPE:]], axis=2).reshape(
        token_count, heads_dev * (LATENT + ROPE)
    )
    absorbed = lax.all_gather(mine, "ctx", axis=0, tiled=True).reshape(-1, heads_dev, LATENT + ROPE)
    highest, totals, head_out = local_attention(absorbed, latent_cache, cache_len[0], up_value)
    all_rows = absorbed.shape[0]
    got_out, got_high, got_total = (
        lax.all_to_all(
            head_out.reshape(all_rows, heads_dev * VDIM),
            "ctx",
            split_axis=0,
            concat_axis=0,
            tiled=True,
        ),
        lax.all_to_all(highest, "ctx", split_axis=0, concat_axis=0, tiled=True),
        lax.all_to_all(totals, "ctx", split_axis=0, concat_axis=0, tiled=True),
    )
    got_out = got_out.reshape(ctx_count, token_count, heads_dev, VDIM)
    got_high = got_high.reshape(ctx_count, token_count, heads_dev)
    got_total = got_total.reshape(ctx_count, token_count, heads_dev)
    overall = jnp.max(got_high, axis=0)
    factor = jnp.exp(got_high - overall[None])
    numerator = jnp.sum(got_out * factor[:, :, :, None], axis=0)
    denominator = jnp.sum(got_total * factor, axis=0)
    attention = (
        (numerator / denominator[:, :, None])
        .astype(jnp.bfloat16)
        .reshape(token_count, heads_dev * VDIM)
    )
    projected = jnp.dot(
        attention,
        lax.all_gather(o_weight, "ctx", axis=1, tiled=True),
        preferred_element_type=jnp.float32,
    )
    quarter = D // sub_count
    offset_cols = lax.axis_index("sub") * quarter
    hidden = residual.astype(jnp.float32) + lax.psum(projected.astype(jnp.bfloat16), "sub").astype(
        jnp.float32
    )
    inverse_rms = lax.rsqrt(jnp.mean(hidden * hidden, axis=1) + epsilon)
    normed = (hidden * inverse_rms[:, None] * norm_gain.astype(jnp.float32)).astype(jnp.bfloat16)
    hidden_part = lax.dynamic_slice_in_dim(hidden, offset_cols, quarter, 1)
    experts_dev = w_gate.shape[0]
    expert_total = experts_dev * ctx_count
    pair_count = token_count * TOP
    expert_ids = route_ids.reshape(pair_count)
    onehot = (expert_ids[:, None] == lax.broadcasted_iota(jnp.int32, (1, expert_total), 1)).astype(
        jnp.int32
    )
    earlier = jnp.cumsum(onehot, axis=0) - onehot
    slot_ids = jnp.sum(earlier * onehot, axis=1)
    targets = (expert_ids * CAP + slot_ids).reshape(token_count, TOP)
    matches = targets[:, :, None] == lax.broadcasted_iota(jnp.int32, (1, 1, expert_total * CAP), 2)
    select = jnp.sum(matches.astype(jnp.int32), axis=1).astype(jnp.bfloat16)
    outgoing = jnp.einsum("tj,td->jd", select, normed, preferred_element_type=jnp.float32).astype(
        jnp.bfloat16
    )
    outgoing = outgoing.reshape(ctx_count, experts_dev, CAP, D)
    received = lax.all_to_all(outgoing, "ctx", split_axis=0, concat_axis=0, tiled=True)
    gate_act = jnp.einsum("sekd,edf->sekf", received, w_gate, preferred_element_type=jnp.float32)
    up_act = jnp.einsum("sekd,edf->sekf", received, w_up, preferred_element_type=jnp.float32)
    gated_rows = (jax.nn.silu(gate_act) * up_act).astype(jnp.bfloat16)
    partial_out = jnp.einsum(
        "sekf,efd->sekd", gated_rows, w_down, preferred_element_type=jnp.float32
    )
    summed = lax.psum_scatter(
        partial_out.astype(jnp.bfloat16), "sub", scatter_dimension=3, tiled=True
    )
    back_rows = lax.all_to_all(summed, "ctx", split_axis=0, concat_axis=0, tiled=True)
    back_rows = back_rows.reshape(expert_total * CAP, quarter)
    mixing = jnp.sum(jnp.where(matches, route_weights[:, :, None], 0.0), axis=1)
    routed = jnp.dot(mixing, back_rows.astype(jnp.float32), precision=lax.Precision.HIGHEST)
    return (hidden_part + routed).astype(jnp.bfloat16)


LANES = 128
TILE = 256
CHUNKS = 1
MESH = pl.DeviceIdType.MESH
F32 = jnp.float32
BF16 = jnp.bfloat16
NT = (((1,), (1,)), ((), ()))


def fused_kernel(
    dims,
    q_hbm,
    res_hbm,
    ids_hbm,
    mix_hbm,
    len_hbm,
    cache_hbm,
    kv_hbm,
    o_hbm,
    gain_hbm,
    gate_hbm,
    up_hbm,
    down_hbm,
    out_ref,
    res_ref,
    ids_ref,
    mix_ref,
    len_ref,
    cache_ref,
    kv_ref,
    o_ref,
    gain_ref,
    q_all,
    res_all,
    comb_send,
    comb_all,
    ql_all,
    lat_send,
    lat_all,
    stat_all,
    att_all,
    proj_send,
    proj_all,
    hid_all,
    normed,
    mix_cols,
    gated,
    fin_send,
    fin_all,
    gate_buf,
    up_buf,
    down_buf,
    in_sem,
    w_sem,
    ctx_send,
    ctx_recv,
    comb_ssem,
    comb_rsem,
    sub_send,
    sub_recv,
    hid_ssem,
    hid_rsem,
    fin_ssem,
    fin_rsem,
):
    grp, ctx, sub, tok, heads, experts = dims
    me_g = lax.axis_index("grp")
    me_c = lax.axis_index("ctx")
    me_s = lax.axis_index("sub")
    span = ctx * tok
    rows = heads * span
    chunk = rows // CHUNKS
    chunk_heads = heads // CHUNKS
    quarter = o_ref.shape[1]
    hidden_units = gate_hbm.shape[1]

    barrier = pltpu.get_barrier_semaphore()

    def everyone():
        for dg in range(grp):
            for dc in range(ctx):
                for ds in range(sub):
                    if dg or dc or ds:
                        yield (
                            (dg * ctx + dc) * sub + ds,
                            lax.rem(me_g + dg, grp),
                            lax.rem(me_c + dc, ctx),
                            lax.rem(me_s + ds, sub),
                        )

    for _, pg, pc, ps in everyone():
        pl.semaphore_signal(
            barrier,
            inc=1,
            device_id={"grp": pg, "ctx": pc, "sub": ps},
            device_id_type=MESH,
        )

    loads = [
        pltpu.make_async_copy(source, target, in_sem.at[i])
        for i, (source, target) in enumerate(
            (
                (q_hbm, q_all.at[me_c]),
                (kv_hbm, kv_ref),
                (res_hbm, res_ref),
                (ids_hbm, ids_ref),
                (mix_hbm, mix_ref),
                (len_hbm, len_ref),
                (cache_hbm, cache_ref),
                (o_hbm, o_ref),
                (gain_hbm, gain_ref),
            )
        )
    ]
    q_load, kv_load, res_load, ids_load, mix_load, len_load, cache_load, o_load, gain_load = loads
    for load in loads:
        load.start()

    weight_loads = []
    for e in range(experts):
        place = pl.ds(e * hidden_units, hidden_units)
        for i, (source, target) in enumerate(
            ((gate_hbm, gate_buf), (up_hbm, up_buf), (down_hbm, down_buf))
        ):
            weight_loads.append(
                pltpu.make_async_copy(
                    source.at[me_g * experts + e], target.at[place], w_sem.at[e, i]
                )
            )
            weight_loads[-1].start()

    def ctx_copies(phase, source_of, target):
        copies = []
        for d in range(1, ctx):
            peer = lax.rem(me_c + d, ctx)
            copies.append(
                pltpu.make_async_remote_copy(
                    src_ref=source_of(peer),
                    dst_ref=target,
                    send_sem=ctx_send.at[phase, d],
                    recv_sem=ctx_recv.at[phase, d],
                    device_id={"ctx": peer},
                    device_id_type=MESH,
                )
            )
            copies[-1].start()
        return copies

    def finish(copies):
        for copy in copies:
            copy.wait()

    q_load.wait()
    pl.semaphore_wait(barrier, grp * ctx * sub - 1)

    q_copies = ctx_copies(0, lambda peer: q_all.at[me_c], q_all.at[me_c])

    res_load.wait()
    piece = quarter // sub

    def own_piece(peer):
        return pl.ds(pl.multiple_of(peer * quarter + me_s * piece, piece), piece)

    early = ctx_copies(1, lambda peer: res_ref.at[:, own_piece(peer)], res_all.at[me_c])
    res_all[me_c] = res_ref[:, own_piece(me_c)]

    ids_load.wait()
    mix_load.wait()
    lane = lax.broadcasted_iota(jnp.int32, (tok, LANES), 1)
    ids, mixes = ids_ref[...], mix_ref[...]
    for c in range(ctx):
        for g in range(grp):
            first = (c * grp + g) * experts
            comb = jnp.zeros((tok, LANES), F32)
            for k in range(TOP):
                hit = (ids[:, k : k + 1] == lane + first) & (lane < experts)
                comb += jnp.where(hit, mixes[:, k : k + 1], 0.0)
            comb_send[g * ctx + c] = comb
    comb_all[me_g * ctx + me_c] = comb_send[me_g * ctx + me_c]
    for dg in range(grp):
        for dc in range(ctx):
            if dg or dc:
                pg, pc = lax.rem(me_g + dg, grp), lax.rem(me_c + dc, ctx)
                early.append(
                    pltpu.make_async_remote_copy(
                        src_ref=comb_send.at[pg * ctx + pc],
                        dst_ref=comb_all.at[me_g * ctx + me_c],
                        send_sem=comb_ssem.at[dg * ctx + dc],
                        recv_sem=comb_rsem.at[dg * ctx + dc],
                        device_id={"grp": pg, "ctx": pc},
                        device_id_type=MESH,
                    )
                )
                early[-1].start()

    kv_load.wait()
    finish(q_copies)
    per_head = NOPE + ROPE
    q_rows = q_all[...].astype(F32).reshape(span, heads * per_head)
    turned = [
        q_rows if h == 0 else pltpu.roll(q_rows, (heads - h) * per_head, 1) for h in range(heads)
    ]
    ql_copies = []
    for k in range(CHUNKS):
        for h in range(k * chunk_heads, (k + 1) * chunk_heads):
            nope = turned[h][:, :NOPE].astype(BF16)
            part = jnp.dot(nope, kv_ref[h, :NOPE, :], preferred_element_type=F32).astype(BF16)
            ql_all[me_c, h * span : (h + 1) * span, :] = part
        block = ql_all.at[me_c, pl.ds(k * chunk, chunk)]
        ql_copies.append(ctx_copies(2 + k, lambda peer: block, block))

    cache_load.wait()
    len_load.wait()
    position = lax.broadcasted_iota(jnp.int32, (1, cache_ref.shape[1]), 1)
    live = position < len_ref[0]
    rope_scores = []
    for k in range(CHUNKS):
        rope = jnp.concatenate(
            [
                turned[h][:, NOPE:per_head]
                for h in range(k * chunk_heads, (k + 1) * chunk_heads)
            ],
            axis=0,
        ).astype(BF16)
        rope_scores.append(jnp.dot(rope, cache_ref[LATENT:, :], preferred_element_type=F32))

    lat_copies = []
    for k in range(CHUNKS):
        finish(ql_copies[k])
        part = slice(k * chunk, (k + 1) * chunk)
        lat_q = jnp.concatenate([ql_all[c, part, :] for c in range(ctx)], axis=1)
        scores = jnp.dot(lat_q, cache_ref[:LATENT, :], preferred_element_type=F32)
        scores = (scores + rope_scores[k]) * (NOPE + ROPE) ** (-0.5)
        scores = jnp.where(live, scores, -jnp.inf)
        highest = jnp.max(scores, axis=1, keepdims=True)
        weights = jnp.exp(scores - highest).astype(BF16)
        latent = lax.dot_general(
            weights, cache_ref[:LATENT, :], NT, preferred_element_type=F32
        ).astype(BF16)
        for c in range(ctx):
            lat_send[c, part, :] = latent[:, c * LANES : (c + 1) * LANES]
        block = pl.ds(k * chunk, chunk)
        copies = ctx_copies(
            2 + CHUNKS + k,
            lambda peer: lat_send.at[peer, block],
            lat_all.at[me_c, block],
        )
        lat_all[me_c, part, :] = lat_send[me_c, part, :]
        totals = jnp.sum(weights.astype(F32), axis=1, keepdims=True)
        side = lax.broadcasted_iota(jnp.int32, (chunk, LANES), 1)
        stats = jnp.where(side < 4, highest, totals).T
        stat_all[me_c, k] = stats[0:8, :]
        copies += ctx_copies(
            2 + 2 * CHUNKS + k, lambda peer: stat_all.at[me_c, k], stat_all.at[me_c, k]
        )
        lat_copies.append(copies)

    att_copies = []
    for k in range(CHUNKS):
        finish(lat_copies[k])
        part = slice(k * chunk, (k + 1) * chunk)
        highs = [stat_all[c, k, 0:1, :] for c in range(ctx)]
        overall = functools.reduce(jnp.maximum, highs)
        factors = [jnp.exp(high - overall) for high in highs]
        denominator = sum(f * stat_all[c, k, 4:5, :] for c, f in enumerate(factors))
        merged = jnp.zeros((chunk, LANES), F32)
        for c in range(ctx):
            scale = jnp.broadcast_to(factors[c] / denominator, (LANES, chunk)).T
            merged += lat_all[c, part, :].astype(F32) * scale
        merged = merged.astype(BF16)
        for j in range(chunk_heads):
            h = k * chunk_heads + j
            out = lax.dot_general(
                merged[j * span : (j + 1) * span, :],
                kv_ref[h, NOPE:, :],
                NT,
                preferred_element_type=F32,
            )
            att_all[me_c, k, :, j * VDIM : (j + 1) * VDIM] = out.astype(BF16)
        block = att_all.at[me_c, k]
        att_copies.append(ctx_copies(2 + 3 * CHUNKS + k, lambda peer: block, block))

    o_load.wait()
    width = chunk_heads * VDIM
    projected = jnp.zeros((span, quarter), F32)
    for k in range(CHUNKS):
        finish(att_copies[k])
        attention = sum(att_all[c, k].astype(F32) for c in range(ctx)).astype(BF16)
        projected += jnp.dot(
            attention, o_ref[k * width : (k + 1) * width, :], preferred_element_type=F32
        )
    for s in range(sub):
        proj_send[s] = projected[:, s * piece : (s + 1) * piece].astype(BF16)
    copies = []
    for d in range(1, sub):
        peer = lax.rem(me_s + d, sub)
        copies.append(
            pltpu.make_async_remote_copy(
                src_ref=proj_send.at[peer],
                dst_ref=proj_all.at[me_s],
                send_sem=sub_send.at[d],
                recv_sem=sub_recv.at[d],
                device_id={"sub": peer},
                device_id_type=MESH,
            )
        )
        copies[-1].start()
    proj_all[me_s] = proj_send[me_s]
    finish(early)

    comb = comb_all[...].reshape(grp * span, LANES)
    comb_lane = lax.broadcasted_iota(jnp.int32, (grp * span, LANES), 1)
    columns = [
        jnp.sum(jnp.where(comb_lane == e, comb, 0.0), axis=1, keepdims=True)
        for e in range(experts)
    ]
    for t in range(experts * hidden_units // LANES):
        low, high = t * LANES // hidden_units, (t * LANES + LANES - 1) // hidden_units
        mix = jnp.broadcast_to(columns[low], (grp * span, LANES))
        if high > low:
            mix = jnp.where(comb_lane < high * hidden_units - t * LANES, mix, columns[high])
        mix_cols[:, t * LANES : (t + 1) * LANES] = mix

    residual = res_all[...].astype(F32).reshape(span, piece)
    finish(copies)
    me = (me_g * ctx + me_c) * sub + me_s
    hid_all[me] = (residual + sum(proj_all[s].astype(F32) for s in range(sub))).astype(BF16)
    copies = []
    for i, pg, pc, ps in everyone():
        copies.append(
            pltpu.make_async_remote_copy(
                src_ref=hid_all.at[me],
                dst_ref=hid_all.at[me],
                send_sem=hid_ssem.at[i],
                recv_sem=hid_rsem.at[i],
                device_id={"grp": pg, "ctx": pc, "sub": ps},
                device_id_type=MESH,
            )
        )
        copies[-1].start()
    gain_load.wait()
    gain = gain_ref[...].astype(F32)
    finish(copies)

    parts = ctx * sub
    for g in range(grp):
        own = slice(g * span, (g + 1) * span)
        pieces = [hid_all[g * parts + j].astype(F32) for j in range(parts)]
        squares = jnp.sum(sum(p * p for p in pieces), axis=1, keepdims=True)
        inverse_rms = lax.rsqrt(squares / (parts * piece) + epsilon)
        for j in range(parts):
            normed[own, j * piece : (j + 1) * piece] = (
                pieces[j] * inverse_rms * gain[j : j + 1, :]
            ).astype(BF16)

    finish(weight_loads)
    for t in range(experts * hidden_units // TILE):
        tile = slice(t * TILE, (t + 1) * TILE)
        gate_act = lax.dot_general(gate_buf[tile, :], normed[...], NT, preferred_element_type=F32)
        up_act = lax.dot_general(up_buf[tile, :], normed[...], NT, preferred_element_type=F32)
        both = gate_act / (1.0 + jnp.exp(-gate_act)) * up_act
        gated[:, tile] = (both.T * mix_cols[:, tile]).astype(BF16)

    copies = []
    for ds in range(sub):
        ps = lax.rem(me_s + ds, sub)
        cols = pl.ds(pl.multiple_of(ps * quarter, quarter), quarter)
        block = jnp.dot(gated[...], down_buf[:, cols], preferred_element_type=F32).astype(BF16)
        for i in range(grp * ctx):
            fin_send[ds, i] = block[i * tok : (i + 1) * tok, :]
        for dg in range(grp):
            for dc in range(ctx):
                pg, pc = lax.rem(me_g + dg, grp), lax.rem(me_c + dc, ctx)
                if dg or dc or ds:
                    i = (dg * ctx + dc) * sub + ds
                    copies.append(
                        pltpu.make_async_remote_copy(
                            src_ref=fin_send.at[ds, pg * ctx + pc],
                            dst_ref=fin_all.at[me],
                            send_sem=fin_ssem.at[i],
                            recv_sem=fin_rsem.at[i],
                            device_id={"grp": pg, "ctx": pc, "sub": ps},
                            device_id_type=MESH,
                        )
                    )
                    copies[-1].start()
        if ds == 0:
            fin_all[me] = fin_send[0, me_g * ctx + me_c]
    hidden = jnp.concatenate(
        [
            hid_all[(me_g * ctx + me_s) * sub + s].astype(F32)
            for s in range(sub)
        ],
        axis=1,
    )
    mine = jnp.zeros((tok, quarter), F32)
    for c in range(ctx):
        mine += jnp.where(me_c == c, hidden[c * tok : (c + 1) * tok, :], 0.0)
    finish(copies)
    routed = sum(fin_all[i].astype(F32) for i in range(grp * ctx * sub))
    out_ref[...] = (mine + routed).astype(out_ref.dtype)


def fused_body(
    queries,
    latent_cache,
    cache_len,
    kv_up,
    o_weight,
    residual,
    norm_gain,
    route_ids,
    route_weights,
    w_gate,
    w_up,
    w_down,
):
    grp, ctx, sub = lax.axis_size("grp"), lax.axis_size("ctx"), lax.axis_size("sub")
    heads, tok, experts = kv_up.shape[0], queries.shape[0], w_gate.shape[0] // grp
    span, rows, quarter = ctx * tok, heads * ctx * tok, o_weight.shape[1]
    width, piece, everyone = residual.shape[1], quarter // sub, grp * ctx * sub
    w_gate, w_up = jnp.swapaxes(w_gate, 1, 2), jnp.swapaxes(w_up, 1, 2)
    units = experts * w_gate.shape[1]
    cache = latent_cache.T
    gain = norm_gain.reshape(width // LANES, LANES)
    hbm = pl.BlockSpec(memory_space=pl.ANY)
    dma = pltpu.SemaphoreType.DMA
    return pl.pallas_call(
        functools.partial(fused_kernel, (grp, ctx, sub, tok, heads, experts)),
        out_shape=jax.ShapeDtypeStruct((tok, width // sub), BF16),
        in_specs=[hbm] * 12,
        out_specs=pl.BlockSpec(memory_space=pltpu.VMEM),
        scratch_shapes=[
            pltpu.VMEM(residual.shape, BF16),
            pltpu.VMEM(route_ids.shape, jnp.int32),
            pltpu.VMEM(route_weights.shape, F32),
            pltpu.SMEM(cache_len.shape, jnp.int32),
            pltpu.VMEM(cache.shape, BF16),
            pltpu.VMEM(kv_up.shape, BF16),
            pltpu.VMEM(o_weight.shape, BF16),
            pltpu.VMEM(gain.shape, BF16),
            pltpu.VMEM((ctx,) + queries.shape, BF16),
            pltpu.VMEM((ctx, tok, piece), BF16),
            pltpu.VMEM((grp * ctx, tok, LANES), F32),
            pltpu.VMEM((grp * ctx, tok, LANES), F32),
            pltpu.VMEM((ctx, rows, LANES), BF16),
            pltpu.VMEM((ctx, rows, LANES), BF16),
            pltpu.VMEM((ctx, rows, LANES), BF16),
            pltpu.VMEM((ctx, CHUNKS, 8, rows // CHUNKS), F32),
            pltpu.VMEM((ctx, CHUNKS, span, heads * VDIM // CHUNKS), BF16),
            pltpu.VMEM((sub, span, piece), BF16),
            pltpu.VMEM((sub, span, piece), BF16),
            pltpu.VMEM((everyone, span, piece), BF16),
            pltpu.VMEM((grp * span, width), BF16),
            pltpu.VMEM((grp * span, units), F32),
            pltpu.VMEM((grp * span, units), BF16),
            pltpu.VMEM((sub, grp * ctx, tok, quarter), BF16),
            pltpu.VMEM((everyone, tok, quarter), BF16),
            pltpu.VMEM((units, width), BF16),
            pltpu.VMEM((units, width), BF16),
            pltpu.VMEM((units, width), BF16),
            dma((9,)),
            dma((experts, 3)),
            dma((2 + 4 * CHUNKS, ctx)),
            dma((2 + 4 * CHUNKS, ctx)),
            dma((grp * ctx,)),
            dma((grp * ctx,)),
            dma((sub,)),
            dma((sub,)),
            dma((everyone,)),
            dma((everyone,)),
            dma((everyone,)),
            dma((everyone,)),
        ],
        compiler_params=pltpu.CompilerParams(
            collective_id=0, has_side_effects=True, vmem_limit_bytes=56 * 1024 * 1024
        ),
    )(
        queries,
        residual,
        route_ids,
        route_weights,
        cache_len,
        cache,
        kv_up,
        o_weight,
        gain,
        w_gate,
        w_up,
        w_down,
    )


def choose_body(*args):
    kv_up, o_weight, w_gate = args[3], args[4], args[9]
    grp, ctx, sub = lax.axis_size("grp"), lax.axis_size("ctx"), lax.axis_size("sub")
    tok, experts = args[0].shape[0], w_gate.shape[0]
    units = experts // grp * w_gate.shape[2]
    fits = (
        ctx == sub
        and kv_up.shape[2] == LANES
        and o_weight.shape[1] == sub * LANES
        and kv_up.shape[0] * ctx * tok == LANES
        and experts % grp == 0
        and experts <= LANES
        and w_gate.shape[2] % 16 == 0
        and units % TILE == 0
        and units * w_gate.shape[1] * 6 <= 40 * 1024 * 1024
        and tok % 8 == 0
    )
    return fused_body(*args) if fits else body(*args)


def solution(mesh):
    in_specs = (
        P(("grp", "ctx"), "sub"),
        P(("grp", "ctx"), None),
        P(("grp", "ctx")),
        P(("grp", "sub"), None, "ctx"),
        P("sub", "ctx"),
        P(("grp", "ctx"), None),
        P(),
        P(("grp", "ctx"), None),
        P(("grp", "ctx"), None),
        P("ctx", None, "sub"),
        P("ctx", None, "sub"),
        P("ctx", "sub", None),
    )
    out_specs = P(("grp", "ctx"), "sub")
    return jax.shard_map(choose_body, mesh=mesh, in_specs=in_specs, out_specs=out_specs, check_vma=False)
```

```python
import functools

import jax
import jax.numpy as jnp
from jax import lax
from jax.experimental import pallas as pl
from jax.experimental.pallas import tpu as pltpu
from jax.sharding import PartitionSpec as P

D = 2048
NOPE = 128
ROPE = 64
VDIM = 128
LATENT = 512
TOP = 6
CAP = 2


epsilon = 1e-06


def local_attention(absorbed, cache_rows, length, up_value):
    scores = jnp.einsum("qhc,kc->qhk", absorbed, cache_rows, preferred_element_type=jnp.float32) * (
        NOPE + ROPE
    ) ** (-0.5)
    live_mask = lax.broadcasted_iota(jnp.int32, (cache_rows.shape[0],), 0) < length
    scores = jnp.where(live_mask[None, None, :], scores, -jnp.inf)
    highest = jnp.max(scores, axis=2)
    weights = jnp.exp(scores - highest[:, :, None]).astype(jnp.bfloat16)
    totals = jnp.sum(weights, axis=2, dtype=jnp.float32)
    latent_out = jnp.einsum(
        "qhk,kl->qhl", weights, cache_rows[:, :LATENT], preferred_element_type=jnp.float32
    ).astype(jnp.bfloat16)
    head_out = jnp.einsum("qhl,hvl->qhv", latent_out, up_value, preferred_element_type=jnp.float32)
    return (highest, totals, head_out)


def body(
    queries,
    latent_cache,
    cache_len,
    kv_up,
    o_weight,
    residual,
    norm_gain,
    route_ids,
    route_weights,
    w_gate,
    w_up,
    w_down,
):
    ctx_count = lax.axis_size("ctx")
    sub_count = lax.axis_size("sub")
    heads_dev = kv_up.shape[0]
    token_count = queries.shape[0]
    up_full = lax.all_gather(kv_up, "ctx", axis=2, tiled=True)
    up_key = up_full[:, :NOPE, :]
    up_value = up_full[:, NOPE:, :]
    own_rows = queries.reshape(token_count, heads_dev, NOPE + ROPE)
    query_latent = jnp.einsum(
        "qhn,hnl->qhl", own_rows[:, :, :NOPE], up_key, preferred_element_type=jnp.float32
    ).astype(jnp.bfloat16)
    mine = jnp.concatenate([query_latent, own_rows[:, :, NOPE:]], axis=2).reshape(
        token_count, heads_dev * (LATENT + ROPE)
    )
    absorbed = lax.all_gather(mine, "ctx", axis=0, tiled=True).reshape(-1, heads_dev, LATENT + ROPE)
    highest, totals, head_out = local_attention(absorbed, latent_cache, cache_len[0], up_value)
    all_rows = absorbed.shape[0]
    got_out, got_high, got_total = (
        lax.all_to_all(
            head_out.reshape(all_rows, heads_dev * VDIM),
            "ctx",
            split_axis=0,
            concat_axis=0,
            tiled=True,
        ),
        lax.all_to_all(highest, "ctx", split_axis=0, concat_axis=0, tiled=True),
        lax.all_to_all(totals, "ctx", split_axis=0, concat_axis=0, tiled=True),
    )
    got_out = got_out.reshape(ctx_count, token_count, heads_dev, VDIM)
    got_high = got_high.reshape(ctx_count, token_count, heads_dev)
    got_total = got_total.reshape(ctx_count, token_count, heads_dev)
    overall = jnp.max(got_high, axis=0)
    factor = jnp.exp(got_high - overall[None])
    numerator = jnp.sum(got_out * factor[:, :, :, None], axis=0)
    denominator = jnp.sum(got_total * factor, axis=0)
    attention = (
        (numerator / denominator[:, :, None])
        .astype(jnp.bfloat16)
        .reshape(token_count, heads_dev * VDIM)
    )
    projected = jnp.dot(
        attention,
        lax.all_gather(o_weight, "ctx", axis=1, tiled=True),
        preferred_element_type=jnp.float32,
    )
    quarter = D // sub_count
    offset_cols = lax.axis_index("sub") * quarter
    hidden = residual.astype(jnp.float32) + lax.psum(projected.astype(jnp.bfloat16), "sub").astype(
        jnp.float32
    )
    inverse_rms = lax.rsqrt(jnp.mean(hidden * hidden, axis=1) + epsilon)
    normed = (hidden * inverse_rms[:, None] * norm_gain.astype(jnp.float32)).astype(jnp.bfloat16)
    hidden_part = lax.dynamic_slice_in_dim(hidden, offset_cols, quarter, 1)
    experts_dev = w_gate.shape[0]
    expert_total = experts_dev * ctx_count
    pair_count = token_count * TOP
    expert_ids = route_ids.reshape(pair_count)
    onehot = (expert_ids[:, None] == lax.broadcasted_iota(jnp.int32, (1, expert_total), 1)).astype(
        jnp.int32
    )
    earlier = jnp.cumsum(onehot, axis=0) - onehot
    slot_ids = jnp.sum(earlier * onehot, axis=1)
    targets = (expert_ids * CAP + slot_ids).reshape(token_count, TOP)
    matches = targets[:, :, None] == lax.broadcasted_iota(jnp.int32, (1, 1, expert_total * CAP), 2)
    select = jnp.sum(matches.astype(jnp.int32), axis=1).astype(jnp.bfloat16)
    outgoing = jnp.einsum("tj,td->jd", select, normed, preferred_element_type=jnp.float32).astype(
        jnp.bfloat16
    )
    outgoing = outgoing.reshape(ctx_count, experts_dev, CAP, D)
    received = lax.all_to_all(outgoing, "ctx", split_axis=0, concat_axis=0, tiled=True)
    gate_act = jnp.einsum("sekd,edf->sekf", received, w_gate, preferred_element_type=jnp.float32)
    up_act = jnp.einsum("sekd,edf->sekf", received, w_up, preferred_element_type=jnp.float32)
    gated_rows = (jax.nn.silu(gate_act) * up_act).astype(jnp.bfloat16)
    partial_out = jnp.einsum(
        "sekf,efd->sekd", gated_rows, w_down, preferred_element_type=jnp.float32
    )
    summed = lax.psum_scatter(
        partial_out.astype(jnp.bfloat16), "sub", scatter_dimension=3, tiled=True
    )
    back_rows = lax.all_to_all(summed, "ctx", split_axis=0, concat_axis=0, tiled=True)
    back_rows = back_rows.reshape(expert_total * CAP, quarter)
    mixing = jnp.sum(jnp.where(matches, route_weights[:, :, None], 0.0), axis=1)
    routed = jnp.dot(mixing, back_rows.astype(jnp.float32), precision=lax.Precision.HIGHEST)
    return (hidden_part + routed).astype(jnp.bfloat16)


LANES = 128
TILE = 256
CHUNKS = 1
MESH = pl.DeviceIdType.MESH
F32 = jnp.float32
BF16 = jnp.bfloat16
NT = (((1,), (1,)), ((), ()))


def fused_kernel(
    dims,
    q_hbm,
    res_hbm,
    ids_hbm,
    mix_hbm,
    len_hbm,
    cache_hbm,
    kv_hbm,
    o_hbm,
    gain_hbm,
    gate_hbm,
    up_hbm,
    down_hbm,
    out_ref,
    res_ref,
    ids_ref,
    mix_ref,
    len_ref,
    cache_ref,
    kv_ref,
    o_ref,
    gain_ref,
    q_all,
    res_all,
    comb_send,
    comb_all,
    ql_all,
    lat_send,
    lat_all,
    stat_all,
    att_all,
    proj_send,
    proj_all,
    hid_all,
    gain_rows,
    tokens,
    gate_sum,
    up_sum,
    mix_cols,
    gated,
    pair_send,
    pair_all,
    fin_send,
    fin_all,
    gate_buf,
    up_buf,
    down_buf,
    in_sem,
    w_sem,
    ctx_send,
    ctx_recv,
    comb_ssem,
    comb_rsem,
    sub_send,
    sub_recv,
    hid_ssem,
    hid_rsem,
    pair_ssem,
    pair_rsem,
    fin_ssem,
    fin_rsem,
):
    grp, ctx, sub, tok, heads, experts = dims
    me_g = lax.axis_index("grp")
    me_c = lax.axis_index("ctx")
    me_s = lax.axis_index("sub")
    span = ctx * tok
    rows = heads * span
    chunk = rows // CHUNKS
    chunk_heads = heads // CHUNKS
    quarter = o_ref.shape[1]
    hidden_units = gate_hbm.shape[1]

    barrier = pltpu.get_barrier_semaphore()

    def everyone():
        for dg in range(grp):
            for dc in range(ctx):
                for ds in range(sub):
                    if dg or dc or ds:
                        yield (
                            (dg * ctx + dc) * sub + ds,
                            lax.rem(me_g + dg, grp),
                            lax.rem(me_c + dc, ctx),
                            lax.rem(me_s + ds, sub),
                        )

    for _, pg, pc, ps in everyone():
        pl.semaphore_signal(
            barrier,
            inc=1,
            device_id={"grp": pg, "ctx": pc, "sub": ps},
            device_id_type=MESH,
        )

    loads = [
        pltpu.make_async_copy(source, target, in_sem.at[i])
        for i, (source, target) in enumerate(
            (
                (q_hbm, q_all.at[me_c]),
                (kv_hbm, kv_ref),
                (res_hbm, res_ref),
                (ids_hbm, ids_ref),
                (mix_hbm, mix_ref),
                (len_hbm, len_ref),
                (cache_hbm, cache_ref),
                (o_hbm, o_ref),
                (gain_hbm, gain_ref),
            )
        )
    ]
    q_load, kv_load, res_load, ids_load, mix_load, len_load, cache_load, o_load, gain_load = loads
    for load in loads:
        load.start()

    weight_loads = []
    for e in range(experts):
        place = pl.ds(e * hidden_units, hidden_units)
        for i, (source, target) in enumerate(
            ((gate_hbm, gate_buf), (up_hbm, up_buf), (down_hbm, down_buf))
        ):
            weight_loads.append(
                pltpu.make_async_copy(
                    source.at[me_g * experts + e], target.at[place], w_sem.at[e, i]
                )
            )
            weight_loads[-1].start(priority=1)

    upper = me_c // (ctx // 2)
    sends = []

    def far(i):
        low = ctx - 1 - i
        low = low - (me_c - low + ctx) // ctx
        high = i + (i - me_c + ctx) // ctx
        return low + upper * (high - low)

    far_first = [far(i) for i in range(ctx - 1)]
    near_first = far_first[::-1]

    def send(source, target, send_sem, recv_sem, **peer):
        copy = pltpu.make_async_remote_copy(
            src_ref=source,
            dst_ref=target,
            send_sem=send_sem,
            recv_sem=recv_sem,
            device_id=peer,
            device_id_type=MESH,
        )
        copy.start()
        sends.append(copy)

    def arrived(target, recv_sem):
        pltpu.make_async_remote_copy(
            src_ref=target,
            dst_ref=target,
            send_sem=sub_send.at[0],
            recv_sem=recv_sem,
            device_id={"ctx": far_first[0]},
            device_id_type=MESH,
        ).wait_recv()

    def ctx_copies(phase, source_of, target_of):
        for i, peer in enumerate(far_first):
            send(
                source_of(peer),
                target_of(me_c),
                ctx_send.at[phase, i],
                ctx_recv.at[phase, me_c],
                ctx=peer,
            )
        return [(target_of(peer), ctx_recv.at[phase, peer]) for peer in near_first]

    def finish(arrivals):
        for arrival in arrivals:
            arrived(*arrival)

    q_load.wait()
    pl.semaphore_wait(barrier, grp * ctx * sub - 1)

    q_copies = ctx_copies(0, lambda peer: q_all.at[me_c], lambda c: q_all.at[c])

    res_load.wait()
    piece = quarter // sub

    def own_piece(peer):
        return pl.ds(pl.multiple_of(peer * quarter + me_s * piece, piece), piece)

    early = ctx_copies(
        1, lambda peer: res_ref.at[:, own_piece(peer)], lambda c: res_all.at[c]
    )
    res_all[me_c] = res_ref[:, own_piece(me_c)]

    ids_load.wait()
    mix_load.wait()
    lane = lax.broadcasted_iota(jnp.int32, (tok, LANES), 1)
    ids, mixes = ids_ref[...], mix_ref[...]
    for c in range(ctx):
        for g in range(grp):
            first = (c * grp + g) * experts
            comb = jnp.zeros((tok, LANES), F32)
            for k in range(TOP):
                hit = (ids[:, k : k + 1] == lane + first) & (lane < experts)
                comb += jnp.where(hit, mixes[:, k : k + 1], 0.0)
            comb_send[g * ctx + c] = comb
    comb_all[me_g * ctx + me_c] = comb_send[me_g * ctx + me_c]
    me_gc = me_g * ctx + me_c
    for dg in range(grp):
        pg = lax.rem(me_g + dg, grp)
        for i, pc in enumerate(far_first if dg == 0 else far_first + [me_c]):
            send(
                comb_send.at[pg * ctx + pc],
                comb_all.at[me_gc],
                comb_ssem.at[dg * ctx + i],
                comb_rsem.at[me_gc],
                grp=pg,
                ctx=pc,
            )
            early.append((comb_all.at[pg * ctx + pc], comb_rsem.at[pg * ctx + pc]))

    kv_load.wait()
    finish(q_copies)
    per_head = NOPE + ROPE
    q_rows = q_all[...].astype(F32).reshape(span, heads * per_head)
    turned = [
        q_rows if h == 0 else pltpu.roll(q_rows, (heads - h) * per_head, 1) for h in range(heads)
    ]
    ql_copies = []
    for k in range(CHUNKS):
        for h in range(k * chunk_heads, (k + 1) * chunk_heads):
            nope = turned[h][:, :NOPE].astype(BF16)
            part = jnp.dot(nope, kv_ref[h, :NOPE, :], preferred_element_type=F32).astype(BF16)
            ql_all[me_c, h * span : (h + 1) * span, :] = part
        block = pl.ds(k * chunk, chunk)
        ql_copies.append(
            ctx_copies(2 + k, lambda peer: ql_all.at[me_c, block], lambda c: ql_all.at[c, block])
        )

    cache_load.wait()
    len_load.wait()
    position = lax.broadcasted_iota(jnp.int32, (1, cache_ref.shape[1]), 1)
    live = position < len_ref[0]
    rope_scores = []
    for k in range(CHUNKS):
        rope = jnp.concatenate(
            [
                turned[h][:, NOPE:per_head]
                for h in range(k * chunk_heads, (k + 1) * chunk_heads)
            ],
            axis=0,
        ).astype(BF16)
        rope_scores.append(jnp.dot(rope, cache_ref[LATENT:, :], preferred_element_type=F32))

    lat_copies = []
    for k in range(CHUNKS):
        finish(ql_copies[k])
        part = slice(k * chunk, (k + 1) * chunk)
        lat_q = jnp.concatenate([ql_all[c, part, :] for c in range(ctx)], axis=1)
        scores = jnp.dot(lat_q, cache_ref[:LATENT, :], preferred_element_type=F32)
        scores = (scores + rope_scores[k]) * (NOPE + ROPE) ** (-0.5)
        scores = jnp.where(live, scores, -jnp.inf)
        highest = jnp.max(scores, axis=1, keepdims=True)
        weights = jnp.exp(scores - highest).astype(BF16)
        latent = lax.dot_general(
            weights, cache_ref[:LATENT, :], NT, preferred_element_type=F32
        ).astype(BF16)
        for c in range(ctx):
            lat_send[c, part, :] = latent[:, c * LANES : (c + 1) * LANES]
        block = pl.ds(k * chunk, chunk)
        copies = ctx_copies(
            2 + CHUNKS + k,
            lambda peer: lat_send.at[peer, block],
            lambda c: lat_all.at[c, block],
        )
        lat_all[me_c, part, :] = lat_send[me_c, part, :]
        totals = jnp.sum(weights.astype(F32), axis=1, keepdims=True)
        side = lax.broadcasted_iota(jnp.int32, (chunk, LANES), 1)
        stats = jnp.where(side < 4, highest, totals).T
        stat_all[me_c, k] = stats[0:8, :]
        copies += ctx_copies(
            2 + 2 * CHUNKS + k, lambda peer: stat_all.at[me_c, k], lambda c: stat_all.at[c, k]
        )
        lat_copies.append(copies)

    att_copies = []
    for k in range(CHUNKS):
        finish(lat_copies[k])
        part = slice(k * chunk, (k + 1) * chunk)
        highs = [stat_all[c, k, 0:1, :] for c in range(ctx)]
        overall = functools.reduce(jnp.maximum, highs)
        factors = [jnp.exp(high - overall) for high in highs]
        denominator = sum(f * stat_all[c, k, 4:5, :] for c, f in enumerate(factors))
        merged = jnp.zeros((chunk, LANES), F32)
        for c in range(ctx):
            scale = jnp.broadcast_to(factors[c] / denominator, (LANES, chunk)).T
            merged += lat_all[c, part, :].astype(F32) * scale
        merged = merged.astype(BF16)
        for j in range(chunk_heads):
            h = k * chunk_heads + j
            out = lax.dot_general(
                merged[j * span : (j + 1) * span, :],
                kv_ref[h, NOPE:, :],
                NT,
                preferred_element_type=F32,
            )
            att_all[me_c, k, :, j * VDIM : (j + 1) * VDIM] = out.astype(BF16)
        att_copies.append(
            ctx_copies(
                2 + 3 * CHUNKS + k, lambda peer: att_all.at[me_c, k], lambda c: att_all.at[c, k]
            )
        )

    o_load.wait()
    width = chunk_heads * VDIM
    projected = jnp.zeros((span, quarter), F32)
    for k in range(CHUNKS):
        finish(att_copies[k])
        attention = sum(att_all[c, k].astype(F32) for c in range(ctx)).astype(BF16)
        projected += jnp.dot(
            attention, o_ref[k * width : (k + 1) * width, :], preferred_element_type=F32
        )
    for s in range(sub):
        proj_send[s] = projected[:, s * piece : (s + 1) * piece].astype(BF16)
    copies = []
    for d in range(1, sub):
        peer = lax.rem(me_s + d, sub)
        send(proj_send.at[peer], proj_all.at[me_s], sub_send.at[d], sub_recv.at[me_s], sub=peer)
        copies.append((proj_all.at[peer], sub_recv.at[peer]))
    proj_all[me_s] = proj_send[me_s]
    finish(early)
    gain_load.wait()
    gain_rows[...] = gain_ref[...].astype(F32)

    comb = comb_all[...].reshape(grp * span, LANES)
    comb_lane = lax.broadcasted_iota(jnp.int32, (grp * span, LANES), 1)
    columns = [
        jnp.sum(jnp.where(comb_lane == e, comb, 0.0), axis=1, keepdims=True)
        for e in range(experts)
    ]
    for t in range(experts * hidden_units // LANES):
        low, high = t * LANES // hidden_units, (t * LANES + LANES - 1) // hidden_units
        mix = jnp.broadcast_to(columns[low], (grp * span, LANES))
        if high > low:
            mix = jnp.where(comb_lane < high * hidden_units - t * LANES, mix, columns[high])
        mix_cols[:, t * LANES : (t + 1) * LANES] = mix

    residual = res_all[...].astype(F32).reshape(span, piece)
    finish(copies)
    me = (me_g * ctx + me_c) * sub + me_s
    hid_all[me] = (residual + sum(proj_all[s].astype(F32) for s in range(sub))).astype(BF16)
    count = 0
    for k in range(ctx):
        pc = me_c if k == 0 else near_first[k - 1]
        for dg in range(grp):
            for ds in range(sub):
                if k or dg or ds:
                    send(
                        hid_all.at[me],
                        hid_all.at[me],
                        hid_ssem.at[count],
                        hid_rsem.at[me],
                        grp=lax.rem(me_g + dg, grp),
                        ctx=pc,
                        sub=lax.rem(me_s + ds, sub),
                    )
                    count += 1

    for load in weight_loads:
        load.wait()
    squares = [jnp.zeros((span, piece), F32) for _ in range(grp)]
    tiles = experts * hidden_units // TILE
    for k in range(ctx):
        pc = me_c if k == 0 else near_first[k - 1]
        for dg in range(grp):
            for ds in range(sub):
                if k or dg or ds:
                    at = (lax.rem(me_g + dg, grp) * ctx + pc) * sub + lax.rem(me_s + ds, sub)
                    arrived(hid_all.at[at], hid_rsem.at[at])
        for g in range(grp):
            for t in range(sub):
                block = hid_all[(g * ctx + pc) * sub + t].astype(F32)
                squares[g] += block * block
                scaled = block * gain_rows[pl.ds(pc * sub + t, 1), :]
                tokens[k, g * span : (g + 1) * span, t * piece : (t + 1) * piece] = scaled.astype(
                    BF16
                )
        if k == ctx - 1:
            means = jnp.sum(jnp.concatenate(squares, axis=0), axis=1, keepdims=True) / (
                ctx * quarter
            )
            inverse_rms = jnp.broadcast_to(lax.rsqrt(means + epsilon), (grp * span, LANES)).T[:1, :]
        cols = pl.ds(pl.multiple_of(pc * quarter, quarter), quarter)
        for t in range(tiles):
            tile = slice(t * TILE, (t + 1) * TILE)
            gate_act = lax.dot_general(
                gate_buf[tile, cols], tokens[k], NT, preferred_element_type=F32
            )
            up_act = lax.dot_general(up_buf[tile, cols], tokens[k], NT, preferred_element_type=F32)
            if k > 0:
                gate_act += gate_sum[tile, :]
                up_act += up_sum[tile, :]
            if k < ctx - 1:
                gate_sum[tile, :] = gate_act
                up_sum[tile, :] = up_act
            else:
                gate_act *= inverse_rms
                both = gate_act / (1.0 + jnp.exp(-gate_act)) * (up_act * inverse_rms)
                gated[:, tile] = (both.T * mix_cols[:, tile]).astype(BF16)

    pairs = sub // 2
    me_p, side = me_s // 2, lax.rem(me_s, 2)

    def down(s):
        cols = pl.ds(pl.multiple_of(s * quarter, quarter), quarter)
        return jnp.dot(gated[...], down_buf[:, cols], preferred_element_type=F32)

    turns = [lax.rem(me_p + dp, pairs) for dp in range(1, pairs)] + [me_p]
    for n, pp in enumerate(turns):
        pair_send[n] = down(2 * pp + 1 - side).astype(BF16)
        send(
            pair_send.at[n],
            pair_all.at[pp],
            pair_ssem.at[n],
            pair_rsem.at[pp],
            sub=2 * me_p + 1 - side,
        )
    arrivals = []
    me_half = me_gc * pairs + me_p
    for n, pp in enumerate(turns):
        block = down(2 * pp + side)
        arrived(pair_all.at[pp], pair_rsem.at[pp])
        block = (block + pair_all[pp].astype(F32)).astype(BF16)
        for i in range(grp * ctx):
            fin_send[n, i] = block[i * tok : (i + 1) * tok, :]
        count = 0
        for pc in far_first + [me_c]:
            for dg in range(grp):
                pg = lax.rem(me_g + dg, grp)
                if pc is me_c and dg == 0 and n == pairs - 1:
                    fin_all[me_half] = fin_send[n, me_gc]
                    continue
                send(
                    fin_send.at[n, pg * ctx + pc],
                    fin_all.at[me_half],
                    fin_ssem.at[n * grp * ctx + count],
                    fin_rsem.at[me_half],
                    grp=pg,
                    ctx=pc,
                    sub=2 * pp + side,
                )
                count += 1
                at = (pg * ctx + pc) * pairs + pp
                arrivals.append((fin_all.at[at], fin_rsem.at[at]))
    hidden = jnp.concatenate(
        [hid_all[(me_g * ctx + me_s) * sub + t].astype(F32) for t in range(sub)],
        axis=1,
    )
    mine = jnp.zeros((tok, quarter), F32)
    for c in range(ctx):
        mine += jnp.where(me_c == c, hidden[c * tok : (c + 1) * tok, :], 0.0)
    finish(arrivals)
    routed = sum(fin_all[i].astype(F32) for i in range(grp * ctx * pairs))
    out_ref[...] = (mine + routed).astype(out_ref.dtype)
    for copy in sends:
        copy.wait_send()


def fused_body(
    queries,
    latent_cache,
    cache_len,
    kv_up,
    o_weight,
    residual,
    norm_gain,
    route_ids,
    route_weights,
    w_gate,
    w_up,
    w_down,
):
    grp, ctx, sub = lax.axis_size("grp"), lax.axis_size("ctx"), lax.axis_size("sub")
    heads, tok, experts = kv_up.shape[0], queries.shape[0], w_gate.shape[0] // grp
    span, rows, quarter = ctx * tok, heads * ctx * tok, o_weight.shape[1]
    width, piece, everyone = residual.shape[1], quarter // sub, grp * ctx * sub
    w_gate, w_up = jnp.swapaxes(w_gate, 1, 2), jnp.swapaxes(w_up, 1, 2)
    units = experts * w_gate.shape[1]
    cache = latent_cache.T
    gain = norm_gain.reshape(width // LANES, LANES)
    hbm = pl.BlockSpec(memory_space=pl.ANY)
    dma = pltpu.SemaphoreType.DMA
    return pl.pallas_call(
        functools.partial(fused_kernel, (grp, ctx, sub, tok, heads, experts)),
        out_shape=jax.ShapeDtypeStruct((tok, width // sub), BF16),
        in_specs=[hbm] * 12,
        out_specs=pl.BlockSpec(memory_space=pltpu.VMEM),
        scratch_shapes=[
            pltpu.VMEM(residual.shape, BF16),
            pltpu.VMEM(route_ids.shape, jnp.int32),
            pltpu.VMEM(route_weights.shape, F32),
            pltpu.SMEM(cache_len.shape, jnp.int32),
            pltpu.VMEM(cache.shape, BF16),
            pltpu.VMEM(kv_up.shape, BF16),
            pltpu.VMEM(o_weight.shape, BF16),
            pltpu.VMEM(gain.shape, BF16),
            pltpu.VMEM((ctx,) + queries.shape, BF16),
            pltpu.VMEM((ctx, tok, piece), BF16),
            pltpu.VMEM((grp * ctx, tok, LANES), F32),
            pltpu.VMEM((grp * ctx, tok, LANES), F32),
            pltpu.VMEM((ctx, rows, LANES), BF16),
            pltpu.VMEM((ctx, rows, LANES), BF16),
            pltpu.VMEM((ctx, rows, LANES), BF16),
            pltpu.VMEM((ctx, CHUNKS, 8, rows // CHUNKS), F32),
            pltpu.VMEM((ctx, CHUNKS, span, heads * VDIM // CHUNKS), BF16),
            pltpu.VMEM((sub, span, piece), BF16),
            pltpu.VMEM((sub, span, piece), BF16),
            pltpu.VMEM((everyone, span, piece), BF16),
            pltpu.VMEM(gain.shape, F32),
            pltpu.VMEM((ctx, grp * span, quarter), BF16),
            pltpu.VMEM((units, grp * span), F32),
            pltpu.VMEM((units, grp * span), F32),
            pltpu.VMEM((grp * span, units), F32),
            pltpu.VMEM((grp * span, units), BF16),
            pltpu.VMEM((sub // 2, grp * span, quarter), BF16),
            pltpu.VMEM((sub // 2, grp * span, quarter), BF16),
            pltpu.VMEM((sub // 2, grp * ctx, tok, quarter), BF16),
            pltpu.VMEM((everyone // 2, tok, quarter), BF16),
            pltpu.VMEM((units, width), BF16),
            pltpu.VMEM((units, width), BF16),
            pltpu.VMEM((units, width), BF16),
            dma((9,)),
            dma((experts, 3)),
            dma((2 + 4 * CHUNKS, ctx)),
            dma((2 + 4 * CHUNKS, ctx)),
            dma((grp * ctx,)),
            dma((grp * ctx,)),
            dma((sub,)),
            dma((sub,)),
            dma((everyone,)),
            dma((everyone,)),
            dma((sub // 2,)),
            dma((sub // 2,)),
            dma((everyone // 2,)),
            dma((everyone // 2,)),
        ],
        compiler_params=pltpu.CompilerParams(
            collective_id=0, has_side_effects=True, vmem_limit_bytes=56 * 1024 * 1024
        ),
    )(
        queries,
        residual,
        route_ids,
        route_weights,
        cache_len,
        cache,
        kv_up,
        o_weight,
        gain,
        w_gate,
        w_up,
        w_down,
    )


def choose_body(*args):
    kv_up, o_weight, w_gate = args[3], args[4], args[9]
    grp, ctx, sub = lax.axis_size("grp"), lax.axis_size("ctx"), lax.axis_size("sub")
    tok, experts = args[0].shape[0], w_gate.shape[0]
    units = experts // grp * w_gate.shape[2]
    fits = (
        ctx == sub
        and ctx % 2 == 0
        and kv_up.shape[2] == LANES
        and o_weight.shape[1] == sub * LANES
        and kv_up.shape[0] * ctx * tok == LANES
        and experts % grp == 0
        and experts <= LANES
        and w_gate.shape[2] % 16 == 0
        and units % TILE == 0
        and units * w_gate.shape[1] * 6 <= 40 * 1024 * 1024
        and tok % 8 == 0
    )
    return fused_body(*args) if fits else body(*args)


def solution(mesh):
    in_specs = (
        P(("grp", "ctx"), "sub"),
        P(("grp", "ctx"), None),
        P(("grp", "ctx")),
        P(("grp", "sub"), None, "ctx"),
        P("sub", "ctx"),
        P(("grp", "ctx"), None),
        P(),
        P(("grp", "ctx"), None),
        P(("grp", "ctx"), None),
        P("ctx", None, "sub"),
        P("ctx", None, "sub"),
        P("ctx", "sub", None),
    )
    out_specs = P(("grp", "ctx"), "sub")
    return jax.shard_map(choose_body, mesh=mesh, in_specs=in_specs, out_specs=out_specs, check_vma=False)
```

```python
import functools

import jax
import jax.numpy as jnp
from jax import lax
from jax.experimental import pallas as pl
from jax.experimental.pallas import tpu as pltpu
from jax.sharding import PartitionSpec as P

D = 2048
NOPE = 128
ROPE = 64
VDIM = 128
LATENT = 512
TOP = 6
CAP = 2


epsilon = 1e-06


def local_attention(absorbed, cache_rows, length, up_value):
    scores = jnp.einsum("qhc,kc->qhk", absorbed, cache_rows, preferred_element_type=jnp.float32) * (
        NOPE + ROPE
    ) ** (-0.5)
    live_mask = lax.broadcasted_iota(jnp.int32, (cache_rows.shape[0],), 0) < length
    scores = jnp.where(live_mask[None, None, :], scores, -jnp.inf)
    highest = jnp.max(scores, axis=2)
    weights = jnp.exp(scores - highest[:, :, None]).astype(jnp.bfloat16)
    totals = jnp.sum(weights, axis=2, dtype=jnp.float32)
    latent_out = jnp.einsum(
        "qhk,kl->qhl", weights, cache_rows[:, :LATENT], preferred_element_type=jnp.float32
    ).astype(jnp.bfloat16)
    head_out = jnp.einsum("qhl,hvl->qhv", latent_out, up_value, preferred_element_type=jnp.float32)
    return (highest, totals, head_out)


def body(
    queries,
    latent_cache,
    cache_len,
    kv_up,
    o_weight,
    residual,
    norm_gain,
    route_ids,
    route_weights,
    w_gate,
    w_up,
    w_down,
):
    ctx_count = lax.axis_size("ctx")
    sub_count = lax.axis_size("sub")
    heads_dev = kv_up.shape[0]
    token_count = queries.shape[0]
    up_full = lax.all_gather(kv_up, "ctx", axis=2, tiled=True)
    up_key = up_full[:, :NOPE, :]
    up_value = up_full[:, NOPE:, :]
    own_rows = queries.reshape(token_count, heads_dev, NOPE + ROPE)
    query_latent = jnp.einsum(
        "qhn,hnl->qhl", own_rows[:, :, :NOPE], up_key, preferred_element_type=jnp.float32
    ).astype(jnp.bfloat16)
    mine = jnp.concatenate([query_latent, own_rows[:, :, NOPE:]], axis=2).reshape(
        token_count, heads_dev * (LATENT + ROPE)
    )
    absorbed = lax.all_gather(mine, "ctx", axis=0, tiled=True).reshape(-1, heads_dev, LATENT + ROPE)
    highest, totals, head_out = local_attention(absorbed, latent_cache, cache_len[0], up_value)
    all_rows = absorbed.shape[0]
    got_out, got_high, got_total = (
        lax.all_to_all(
            head_out.reshape(all_rows, heads_dev * VDIM),
            "ctx",
            split_axis=0,
            concat_axis=0,
            tiled=True,
        ),
        lax.all_to_all(highest, "ctx", split_axis=0, concat_axis=0, tiled=True),
        lax.all_to_all(totals, "ctx", split_axis=0, concat_axis=0, tiled=True),
    )
    got_out = got_out.reshape(ctx_count, token_count, heads_dev, VDIM)
    got_high = got_high.reshape(ctx_count, token_count, heads_dev)
    got_total = got_total.reshape(ctx_count, token_count, heads_dev)
    overall = jnp.max(got_high, axis=0)
    factor = jnp.exp(got_high - overall[None])
    numerator = jnp.sum(got_out * factor[:, :, :, None], axis=0)
    denominator = jnp.sum(got_total * factor, axis=0)
    attention = (
        (numerator / denominator[:, :, None])
        .astype(jnp.bfloat16)
        .reshape(token_count, heads_dev * VDIM)
    )
    projected = jnp.dot(
        attention,
        lax.all_gather(o_weight, "ctx", axis=1, tiled=True),
        preferred_element_type=jnp.float32,
    )
    quarter = D // sub_count
    offset_cols = lax.axis_index("sub") * quarter
    hidden = residual.astype(jnp.float32) + lax.psum(projected.astype(jnp.bfloat16), "sub").astype(
        jnp.float32
    )
    inverse_rms = lax.rsqrt(jnp.mean(hidden * hidden, axis=1) + epsilon)
    normed = (hidden * inverse_rms[:, None] * norm_gain.astype(jnp.float32)).astype(jnp.bfloat16)
    hidden_part = lax.dynamic_slice_in_dim(hidden, offset_cols, quarter, 1)
    experts_dev = w_gate.shape[0]
    expert_total = experts_dev * ctx_count
    pair_count = token_count * TOP
    expert_ids = route_ids.reshape(pair_count)
    onehot = (expert_ids[:, None] == lax.broadcasted_iota(jnp.int32, (1, expert_total), 1)).astype(
        jnp.int32
    )
    earlier = jnp.cumsum(onehot, axis=0) - onehot
    slot_ids = jnp.sum(earlier * onehot, axis=1)
    targets = (expert_ids * CAP + slot_ids).reshape(token_count, TOP)
    matches = targets[:, :, None] == lax.broadcasted_iota(jnp.int32, (1, 1, expert_total * CAP), 2)
    select = jnp.sum(matches.astype(jnp.int32), axis=1).astype(jnp.bfloat16)
    outgoing = jnp.einsum("tj,td->jd", select, normed, preferred_element_type=jnp.float32).astype(
        jnp.bfloat16
    )
    outgoing = outgoing.reshape(ctx_count, experts_dev, CAP, D)
    received = lax.all_to_all(outgoing, "ctx", split_axis=0, concat_axis=0, tiled=True)
    gate_act = jnp.einsum("sekd,edf->sekf", received, w_gate, preferred_element_type=jnp.float32)
    up_act = jnp.einsum("sekd,edf->sekf", received, w_up, preferred_element_type=jnp.float32)
    gated_rows = (jax.nn.silu(gate_act) * up_act).astype(jnp.bfloat16)
    partial_out = jnp.einsum(
        "sekf,efd->sekd", gated_rows, w_down, preferred_element_type=jnp.float32
    )
    summed = lax.psum_scatter(
        partial_out.astype(jnp.bfloat16), "sub", scatter_dimension=3, tiled=True
    )
    back_rows = lax.all_to_all(summed, "ctx", split_axis=0, concat_axis=0, tiled=True)
    back_rows = back_rows.reshape(expert_total * CAP, quarter)
    mixing = jnp.sum(jnp.where(matches, route_weights[:, :, None], 0.0), axis=1)
    routed = jnp.dot(mixing, back_rows.astype(jnp.float32), precision=lax.Precision.HIGHEST)
    return (hidden_part + routed).astype(jnp.bfloat16)


LANES = 128
TILE = 256
CHUNKS = 1
MESH = pl.DeviceIdType.MESH
F32 = jnp.float32
BF16 = jnp.bfloat16
NT = (((1,), (1,)), ((), ()))


def fused_kernel(
    dims,
    q_hbm,
    res_hbm,
    ids_hbm,
    mix_hbm,
    len_hbm,
    cache_hbm,
    kv_hbm,
    o_hbm,
    gain_hbm,
    gate_hbm,
    up_hbm,
    down_hbm,
    out_ref,
    res_ref,
    ids_ref,
    mix_ref,
    len_ref,
    cache_ref,
    kv_ref,
    o_ref,
    gain_ref,
    q_all,
    res_all,
    comb_send,
    comb_all,
    ql_all,
    lat_send,
    lat_all,
    stat_all,
    att_all,
    proj_send,
    proj_all,
    hid_all,
    gain_rows,
    tokens,
    gate_sum,
    up_sum,
    mix_cols,
    gated,
    pair_send,
    pair_all,
    fin_send,
    fin_all,
    gate_buf,
    up_buf,
    down_buf,
    in_sem,
    w_sem,
    ctx_send,
    ctx_recv,
    comb_ssem,
    comb_rsem,
    sub_send,
    sub_recv,
    hid_ssem,
    hid_rsem,
    pair_ssem,
    pair_rsem,
    fin_ssem,
    fin_rsem,
):
    grp, ctx, sub, tok, heads, experts = dims
    me_g = lax.axis_index("grp")
    me_c = lax.axis_index("ctx")
    me_s = lax.axis_index("sub")
    span = ctx * tok
    rows = heads * span
    chunk = rows // CHUNKS
    chunk_heads = heads // CHUNKS
    quarter = o_ref.shape[1]
    hidden_units = gate_hbm.shape[1]

    barrier = pltpu.get_barrier_semaphore()

    def everyone():
        for dg in range(grp):
            for dc in range(ctx):
                for ds in range(sub):
                    if dg or dc or ds:
                        yield (
                            (dg * ctx + dc) * sub + ds,
                            lax.rem(me_g + dg, grp),
                            lax.rem(me_c + dc, ctx),
                            lax.rem(me_s + ds, sub),
                        )

    for _, pg, pc, ps in everyone():
        pl.semaphore_signal(
            barrier,
            inc=1,
            device_id={"grp": pg, "ctx": pc, "sub": ps},
            device_id_type=MESH,
        )

    loads = [
        pltpu.make_async_copy(source, target, in_sem.at[i])
        for i, (source, target) in enumerate(
            (
                (q_hbm, q_all.at[me_c]),
                (kv_hbm, kv_ref),
                (res_hbm, res_ref),
                (ids_hbm, ids_ref),
                (mix_hbm, mix_ref),
                (len_hbm, len_ref),
                (cache_hbm, cache_ref),
                (o_hbm, o_ref),
                (gain_hbm, gain_ref),
            )
        )
    ]
    q_load, kv_load, res_load, ids_load, mix_load, len_load, cache_load, o_load, gain_load = loads
    for load in loads:
        load.start()

    weight_loads = []
    for e in range(experts):
        place = pl.ds(e * hidden_units, hidden_units)
        for i, (source, target) in enumerate(
            ((gate_hbm, gate_buf), (up_hbm, up_buf), (down_hbm, down_buf))
        ):
            weight_loads.append(
                pltpu.make_async_copy(
                    source.at[me_g * experts + e], target.at[place], w_sem.at[e, i]
                )
            )
            weight_loads[-1].start(priority=1)

    upper = me_c // (ctx // 2)
    sends = []

    def far(i):
        low = ctx - 1 - i
        low = low - (me_c - low + ctx) // ctx
        high = i + (i - me_c + ctx) // ctx
        return low + upper * (high - low)

    far_first = [far(i) for i in range(ctx - 1)]
    near_first = far_first[::-1]

    def send(source, target, send_sem, recv_sem, **peer):
        copy = pltpu.make_async_remote_copy(
            src_ref=source,
            dst_ref=target,
            send_sem=send_sem,
            recv_sem=recv_sem,
            device_id=peer,
            device_id_type=MESH,
        )
        copy.start()
        sends.append(copy)

    def arrived(target, recv_sem):
        pltpu.make_async_remote_copy(
            src_ref=target,
            dst_ref=target,
            send_sem=sub_send.at[0],
            recv_sem=recv_sem,
            device_id={"ctx": far_first[0]},
            device_id_type=MESH,
        ).wait_recv()

    def ctx_copies(phase, source_of, target_of):
        for i, peer in enumerate(far_first):
            send(
                source_of(peer),
                target_of(me_c),
                ctx_send.at[phase, i],
                ctx_recv.at[phase, me_c],
                ctx=peer,
            )
        return [(target_of(peer), ctx_recv.at[phase, peer]) for peer in near_first]

    def finish(arrivals):
        for arrival in arrivals:
            arrived(*arrival)

    q_load.wait()
    pl.semaphore_wait(barrier, grp * ctx * sub - 1)

    q_copies = ctx_copies(0, lambda peer: q_all.at[me_c], lambda c: q_all.at[c])

    res_load.wait()
    piece = quarter // sub

    def own_piece(peer):
        return pl.ds(pl.multiple_of(peer * quarter + me_s * piece, piece), piece)

    early = ctx_copies(
        1, lambda peer: res_ref.at[:, own_piece(peer)], lambda c: res_all.at[c]
    )
    res_all[me_c] = res_ref[:, own_piece(me_c)]

    ids_load.wait()
    mix_load.wait()
    lane = lax.broadcasted_iota(jnp.int32, (tok, LANES), 1)
    ids, mixes = ids_ref[...], mix_ref[...]
    for c in range(ctx):
        for g in range(grp):
            first = (c * grp + g) * experts
            comb = jnp.zeros((tok, LANES), F32)
            for k in range(TOP):
                hit = (ids[:, k : k + 1] == lane + first) & (lane < experts)
                comb += jnp.where(hit, mixes[:, k : k + 1], 0.0)
            comb_send[g * ctx + c] = comb
    comb_all[me_g * ctx + me_c] = comb_send[me_g * ctx + me_c]
    me_gc = me_g * ctx + me_c
    for dg in range(grp):
        pg = lax.rem(me_g + dg, grp)
        for i, pc in enumerate(far_first if dg == 0 else far_first + [me_c]):
            send(
                comb_send.at[pg * ctx + pc],
                comb_all.at[me_gc],
                comb_ssem.at[dg * ctx + i],
                comb_rsem.at[me_gc],
                grp=pg,
                ctx=pc,
            )
            early.append((comb_all.at[pg * ctx + pc], comb_rsem.at[pg * ctx + pc]))

    kv_load.wait()
    finish(q_copies)
    per_head = NOPE + ROPE
    q_rows = q_all[...].astype(F32).reshape(span, heads * per_head)
    turned = [
        q_rows if h == 0 else pltpu.roll(q_rows, (heads - h) * per_head, 1) for h in range(heads)
    ]
    ql_copies = []
    for k in range(CHUNKS):
        for h in range(k * chunk_heads, (k + 1) * chunk_heads):
            nope = turned[h][:, :NOPE].astype(BF16)
            part = jnp.dot(nope, kv_ref[h, :NOPE, :], preferred_element_type=F32).astype(BF16)
            ql_all[me_c, h * span : (h + 1) * span, :] = part
        block = pl.ds(k * chunk, chunk)
        ql_copies.append(
            ctx_copies(2 + k, lambda peer: ql_all.at[me_c, block], lambda c: ql_all.at[c, block])
        )

    cache_load.wait()
    len_load.wait()
    position = lax.broadcasted_iota(jnp.int32, (1, cache_ref.shape[1]), 1)
    live = position < len_ref[0]
    rope_scores = []
    for k in range(CHUNKS):
        rope = jnp.concatenate(
            [
                turned[h][:, NOPE:per_head]
                for h in range(k * chunk_heads, (k + 1) * chunk_heads)
            ],
            axis=0,
        ).astype(BF16)
        rope_scores.append(jnp.dot(rope, cache_ref[LATENT:, :], preferred_element_type=F32))

    lat_copies = []
    for k in range(CHUNKS):
        finish(ql_copies[k])
        part = slice(k * chunk, (k + 1) * chunk)
        lat_q = jnp.concatenate([ql_all[c, part, :] for c in range(ctx)], axis=1)
        scores = jnp.dot(lat_q, cache_ref[:LATENT, :], preferred_element_type=F32)
        scores = (scores + rope_scores[k]) * (NOPE + ROPE) ** (-0.5)
        scores = jnp.where(live, scores, -jnp.inf)
        highest = jnp.max(scores, axis=1, keepdims=True)
        weights = jnp.exp(scores - highest).astype(BF16)
        latent = lax.dot_general(
            weights, cache_ref[:LATENT, :], NT, preferred_element_type=F32
        ).astype(BF16)
        for c in range(ctx):
            lat_send[c, part, :] = latent[:, c * LANES : (c + 1) * LANES]
        block = pl.ds(k * chunk, chunk)
        copies = ctx_copies(
            2 + CHUNKS + k,
            lambda peer: lat_send.at[peer, block],
            lambda c: lat_all.at[c, block],
        )
        lat_all[me_c, part, :] = lat_send[me_c, part, :]
        totals = jnp.sum(weights.astype(F32), axis=1, keepdims=True)
        side = lax.broadcasted_iota(jnp.int32, (chunk, LANES), 1)
        stats = jnp.where(side < 4, highest, totals).T
        stat_all[me_c, k] = stats[0:8, :]
        copies += ctx_copies(
            2 + 2 * CHUNKS + k, lambda peer: stat_all.at[me_c, k], lambda c: stat_all.at[c, k]
        )
        lat_copies.append(copies)

    att_copies = []
    for k in range(CHUNKS):
        finish(lat_copies[k])
        part = slice(k * chunk, (k + 1) * chunk)
        highs = [stat_all[c, k, 0:1, :] for c in range(ctx)]
        overall = functools.reduce(jnp.maximum, highs)
        factors = [jnp.exp(high - overall) for high in highs]
        denominator = sum(f * stat_all[c, k, 4:5, :] for c, f in enumerate(factors))
        merged = jnp.zeros((chunk, LANES), F32)
        for c in range(ctx):
            scale = jnp.broadcast_to(factors[c] / denominator, (LANES, chunk)).T
            merged += lat_all[c, part, :].astype(F32) * scale
        merged = merged.astype(BF16)
        for j in range(chunk_heads):
            h = k * chunk_heads + j
            out = lax.dot_general(
                merged[j * span : (j + 1) * span, :],
                kv_ref[h, NOPE:, :],
                NT,
                preferred_element_type=F32,
            )
            att_all[me_c, k, :, j * VDIM : (j + 1) * VDIM] = out.astype(BF16)
        att_copies.append(
            ctx_copies(
                2 + 3 * CHUNKS + k, lambda peer: att_all.at[me_c, k], lambda c: att_all.at[c, k]
            )
        )

    o_load.wait()
    width = chunk_heads * VDIM
    projected = jnp.zeros((span, quarter), F32)
    for k in range(CHUNKS):
        finish(att_copies[k])
        attention = sum(att_all[c, k].astype(F32) for c in range(ctx)).astype(BF16)
        projected += jnp.dot(
            attention, o_ref[k * width : (k + 1) * width, :], preferred_element_type=F32
        )
    for s in range(sub):
        proj_send[s] = projected[:, s * piece : (s + 1) * piece].astype(BF16)
    copies = []
    for d in range(1, sub):
        peer = lax.rem(me_s + d, sub)
        send(proj_send.at[peer], proj_all.at[me_s], sub_send.at[d], sub_recv.at[me_s], sub=peer)
        copies.append((proj_all.at[peer], sub_recv.at[peer]))
    proj_all[me_s] = proj_send[me_s]
    finish(early)
    gain_load.wait()
    gain_rows[...] = gain_ref[...].astype(F32)

    comb = comb_all[...].reshape(grp * span, LANES)
    comb_lane = lax.broadcasted_iota(jnp.int32, (grp * span, LANES), 1)
    columns = [
        jnp.sum(jnp.where(comb_lane == e, comb, 0.0), axis=1, keepdims=True)
        for e in range(experts)
    ]
    for t in range(experts * hidden_units // LANES):
        low, high = t * LANES // hidden_units, (t * LANES + LANES - 1) // hidden_units
        mix = jnp.broadcast_to(columns[low], (grp * span, LANES))
        if high > low:
            mix = jnp.where(comb_lane < high * hidden_units - t * LANES, mix, columns[high])
        mix_cols[:, t * LANES : (t + 1) * LANES] = mix

    residual = res_all[...].astype(F32).reshape(span, piece)
    finish(copies)
    me = (me_g * ctx + me_c) * sub + me_s
    hid_all[me] = (residual + sum(proj_all[s].astype(F32) for s in range(sub))).astype(BF16)
    def spread(pc, k):
        slot = (me_g * ctx + pc) * sub + me_s
        count = 0
        for dg in range(grp):
            for ds in range(sub):
                if dg or ds:
                    send(
                        hid_all.at[slot],
                        hid_all.at[slot],
                        hid_ssem.at[k * grp * sub + count],
                        hid_rsem.at[slot],
                        grp=lax.rem(me_g + dg, grp),
                        sub=lax.rem(me_s + ds, sub),
                    )
                    count += 1

    for i, pc in enumerate(far_first):
        send(
            hid_all.at[me],
            hid_all.at[me],
            hid_ssem.at[i * grp * sub + grp * sub - 1],
            hid_rsem.at[me],
            ctx=pc,
        )
    spread(me_c, 0)

    def relay(k):
        slot = (me_g * ctx + near_first[k - 1]) * sub + me_s
        arrived(hid_all.at[slot], hid_rsem.at[slot])
        spread(near_first[k - 1], k)

    for load in weight_loads:
        load.wait()
    squares = [jnp.zeros((span, piece), F32) for _ in range(grp)]
    tiles = experts * hidden_units // TILE
    for k in range(ctx):
        pc = me_c if k == 0 else near_first[k - 1]
        for dg in range(grp):
            for ds in range(sub):
                if dg or ds:
                    at = (lax.rem(me_g + dg, grp) * ctx + pc) * sub + lax.rem(me_s + ds, sub)
                    arrived(hid_all.at[at], hid_rsem.at[at])
        for g in range(grp):
            for t in range(sub):
                block = hid_all[(g * ctx + pc) * sub + t].astype(F32)
                squares[g] += block * block
                scaled = block * gain_rows[pl.ds(pc * sub + t, 1), :]
                tokens[k, g * span : (g + 1) * span, t * piece : (t + 1) * piece] = scaled.astype(
                    BF16
                )
        if k == ctx - 1:
            means = jnp.sum(jnp.concatenate(squares, axis=0), axis=1, keepdims=True) / (
                ctx * quarter
            )
            inverse_rms = jnp.broadcast_to(lax.rsqrt(means + epsilon), (grp * span, LANES)).T[:1, :]
        cols = pl.ds(pl.multiple_of(pc * quarter, quarter), quarter)
        for t in range(tiles):
            if k == 0:
                for ahead in range(1, ctx):
                    if t == (ahead - 1) * tiles // ctx:
                        relay(ahead)
            tile = slice(t * TILE, (t + 1) * TILE)
            gate_act = lax.dot_general(
                gate_buf[tile, cols], tokens[k], NT, preferred_element_type=F32
            )
            up_act = lax.dot_general(up_buf[tile, cols], tokens[k], NT, preferred_element_type=F32)
            if k > 0:
                gate_act += gate_sum[tile, :]
                up_act += up_sum[tile, :]
            if k < ctx - 1:
                gate_sum[tile, :] = gate_act
                up_sum[tile, :] = up_act
            else:
                gate_act *= inverse_rms
                both = gate_act / (1.0 + jnp.exp(-gate_act)) * (up_act * inverse_rms)
                gated[:, tile] = (both.T * mix_cols[:, tile]).astype(BF16)

    pairs = sub // 2
    me_p, side = me_s // 2, lax.rem(me_s, 2)

    def down(s):
        cols = pl.ds(pl.multiple_of(s * quarter, quarter), quarter)
        return jnp.dot(gated[...], down_buf[:, cols], preferred_element_type=F32)

    turns = [lax.rem(me_p + dp, pairs) for dp in range(1, pairs)] + [me_p]
    for n, pp in enumerate(turns):
        pair_send[n] = down(2 * pp + 1 - side).astype(BF16)
        send(
            pair_send.at[n],
            pair_all.at[pp],
            pair_ssem.at[n],
            pair_rsem.at[pp],
            sub=2 * me_p + 1 - side,
        )
    arrivals = []
    me_half = me_gc * pairs + me_p
    for n, pp in enumerate(turns):
        block = down(2 * pp + side)
        arrived(pair_all.at[pp], pair_rsem.at[pp])
        block = (block + pair_all[pp].astype(F32)).astype(BF16)
        for i in range(grp * ctx):
            fin_send[n, i] = block[i * tok : (i + 1) * tok, :]
        count = 0
        for pc in far_first + [me_c]:
            for dg in range(grp):
                pg = lax.rem(me_g + dg, grp)
                if pc is me_c and dg == 0 and n == pairs - 1:
                    fin_all[me_half] = fin_send[n, me_gc]
                    continue
                send(
                    fin_send.at[n, pg * ctx + pc],
                    fin_all.at[me_half],
                    fin_ssem.at[n * grp * ctx + count],
                    fin_rsem.at[me_half],
                    grp=pg,
                    ctx=pc,
                    sub=2 * pp + side,
                )
                count += 1
                at = (pg * ctx + pc) * pairs + pp
                arrivals.append((fin_all.at[at], fin_rsem.at[at]))
    hidden = jnp.concatenate(
        [hid_all[(me_g * ctx + me_s) * sub + t].astype(F32) for t in range(sub)],
        axis=1,
    )
    mine = jnp.zeros((tok, quarter), F32)
    for c in range(ctx):
        mine += jnp.where(me_c == c, hidden[c * tok : (c + 1) * tok, :], 0.0)
    finish(arrivals)
    routed = sum(fin_all[i].astype(F32) for i in range(grp * ctx * pairs))
    out_ref[...] = (mine + routed).astype(out_ref.dtype)
    for copy in sends:
        copy.wait_send()


def fused_body(
    queries,
    latent_cache,
    cache_len,
    kv_up,
    o_weight,
    residual,
    norm_gain,
    route_ids,
    route_weights,
    w_gate,
    w_up,
    w_down,
):
    grp, ctx, sub = lax.axis_size("grp"), lax.axis_size("ctx"), lax.axis_size("sub")
    heads, tok, experts = kv_up.shape[0], queries.shape[0], w_gate.shape[0] // grp
    span, rows, quarter = ctx * tok, heads * ctx * tok, o_weight.shape[1]
    width, piece, everyone = residual.shape[1], quarter // sub, grp * ctx * sub
    w_gate, w_up = jnp.swapaxes(w_gate, 1, 2), jnp.swapaxes(w_up, 1, 2)
    units = experts * w_gate.shape[1]
    cache = latent_cache.T
    gain = norm_gain.reshape(width // LANES, LANES)
    hbm = pl.BlockSpec(memory_space=pl.ANY)
    dma = pltpu.SemaphoreType.DMA
    out = pl.pallas_call(
        functools.partial(fused_kernel, (grp, ctx, sub, tok, heads, experts)),
        out_shape=jax.ShapeDtypeStruct((tok, width // sub), F32),
        in_specs=[hbm] * 12,
        out_specs=pl.BlockSpec(memory_space=pltpu.VMEM),
        scratch_shapes=[
            pltpu.VMEM(residual.shape, BF16),
            pltpu.VMEM(route_ids.shape, jnp.int32),
            pltpu.VMEM(route_weights.shape, F32),
            pltpu.SMEM(cache_len.shape, jnp.int32),
            pltpu.VMEM(cache.shape, BF16),
            pltpu.VMEM(kv_up.shape, BF16),
            pltpu.VMEM(o_weight.shape, BF16),
            pltpu.VMEM(gain.shape, BF16),
            pltpu.VMEM((ctx,) + queries.shape, BF16),
            pltpu.VMEM((ctx, tok, piece), BF16),
            pltpu.VMEM((grp * ctx, tok, LANES), F32),
            pltpu.VMEM((grp * ctx, tok, LANES), F32),
            pltpu.VMEM((ctx, rows, LANES), BF16),
            pltpu.VMEM((ctx, rows, LANES), BF16),
            pltpu.VMEM((ctx, rows, LANES), BF16),
            pltpu.VMEM((ctx, CHUNKS, 8, rows // CHUNKS), F32),
            pltpu.VMEM((ctx, CHUNKS, span, heads * VDIM // CHUNKS), BF16),
            pltpu.VMEM((sub, span, piece), BF16),
            pltpu.VMEM((sub, span, piece), BF16),
            pltpu.VMEM((everyone, span, piece), BF16),
            pltpu.VMEM(gain.shape, F32),
            pltpu.VMEM((ctx, grp * span, quarter), BF16),
            pltpu.VMEM((units, grp * span), F32),
            pltpu.VMEM((units, grp * span), F32),
            pltpu.VMEM((grp * span, units), F32),
            pltpu.VMEM((grp * span, units), BF16),
            pltpu.VMEM((sub // 2, grp * span, quarter), BF16),
            pltpu.VMEM((sub // 2, grp * span, quarter), BF16),
            pltpu.VMEM((sub // 2, grp * ctx, tok, quarter), BF16),
            pltpu.VMEM((everyone // 2, tok, quarter), BF16),
            pltpu.VMEM((units, width), BF16),
            pltpu.VMEM((units, width), BF16),
            pltpu.VMEM((units, width), BF16),
            dma((9,)),
            dma((experts, 3)),
            dma((2 + 4 * CHUNKS, ctx)),
            dma((2 + 4 * CHUNKS, ctx)),
            dma((grp * ctx,)),
            dma((grp * ctx,)),
            dma((sub,)),
            dma((sub,)),
            dma((everyone,)),
            dma((everyone,)),
            dma((sub // 2,)),
            dma((sub // 2,)),
            dma((everyone // 2,)),
            dma((everyone // 2,)),
        ],
        compiler_params=pltpu.CompilerParams(
            collective_id=0, has_side_effects=True, vmem_limit_bytes=46 * 1024 * 1024
        ),
    )(
        *(
            operand
            if operand is cache_len
            else pltpu.with_memory_space_constraint(operand, pltpu.HBM)
            for operand in (
                queries,
                residual,
                route_ids,
                route_weights,
                cache_len,
                cache,
                kv_up,
                o_weight,
                gain,
                w_gate,
                w_up,
                w_down,
            )
        )
    )
    return out.astype(BF16)


def choose_body(*args):
    kv_up, o_weight, w_gate = args[3], args[4], args[9]
    grp, ctx, sub = lax.axis_size("grp"), lax.axis_size("ctx"), lax.axis_size("sub")
    tok, experts = args[0].shape[0], w_gate.shape[0]
    units = experts // grp * w_gate.shape[2]
    fits = (
        ctx == sub
        and ctx % 2 == 0
        and kv_up.shape[2] == LANES
        and o_weight.shape[1] == sub * LANES
        and kv_up.shape[0] * ctx * tok == LANES
        and experts % grp == 0
        and experts <= LANES
        and w_gate.shape[2] % 16 == 0
        and units % TILE == 0
        and units * w_gate.shape[1] * 6 <= 40 * 1024 * 1024
        and tok % 8 == 0
    )
    return fused_body(*args) if fits else body(*args)


def solution(mesh):
    in_specs = (
        P(("grp", "ctx"), "sub"),
        P(("grp", "ctx"), None),
        P(("grp", "ctx")),
        P(("grp", "sub"), None, "ctx"),
        P("sub", "ctx"),
        P(("grp", "ctx"), None),
        P(),
        P(("grp", "ctx"), None),
        P(("grp", "ctx"), None),
        P("ctx", None, "sub"),
        P("ctx", None, "sub"),
        P("ctx", "sub", None),
    )
    out_specs = P(("grp", "ctx"), "sub")
    return jax.shard_map(choose_body, mesh=mesh, in_specs=in_specs, out_specs=out_specs, check_vma=False)
```

```python
import functools

import jax
import jax.numpy as jnp
from jax import lax
from jax.experimental import pallas as pl
from jax.experimental.pallas import tpu as pltpu
from jax.sharding import PartitionSpec as P

D = 2048
NOPE = 128
ROPE = 64
VDIM = 128
LATENT = 512
TOP = 6
CAP = 2


epsilon = 1e-06


def local_attention(absorbed, cache_rows, length, up_value):
    scores = jnp.einsum("qhc,kc->qhk", absorbed, cache_rows, preferred_element_type=jnp.float32) * (
        NOPE + ROPE
    ) ** (-0.5)
    live_mask = lax.broadcasted_iota(jnp.int32, (cache_rows.shape[0],), 0) < length
    scores = jnp.where(live_mask[None, None, :], scores, -jnp.inf)
    highest = jnp.max(scores, axis=2)
    weights = jnp.exp(scores - highest[:, :, None]).astype(jnp.bfloat16)
    totals = jnp.sum(weights, axis=2, dtype=jnp.float32)
    latent_out = jnp.einsum(
        "qhk,kl->qhl", weights, cache_rows[:, :LATENT], preferred_element_type=jnp.float32
    ).astype(jnp.bfloat16)
    head_out = jnp.einsum("qhl,hvl->qhv", latent_out, up_value, preferred_element_type=jnp.float32)
    return (highest, totals, head_out)


def body(
    queries,
    latent_cache,
    cache_len,
    kv_up,
    o_weight,
    residual,
    norm_gain,
    route_ids,
    route_weights,
    w_gate,
    w_up,
    w_down,
):
    ctx_count = lax.axis_size("ctx")
    sub_count = lax.axis_size("sub")
    heads_dev = kv_up.shape[0]
    token_count = queries.shape[0]
    up_full = lax.all_gather(kv_up, "ctx", axis=2, tiled=True)
    up_key = up_full[:, :NOPE, :]
    up_value = up_full[:, NOPE:, :]
    own_rows = queries.reshape(token_count, heads_dev, NOPE + ROPE)
    query_latent = jnp.einsum(
        "qhn,hnl->qhl", own_rows[:, :, :NOPE], up_key, preferred_element_type=jnp.float32
    ).astype(jnp.bfloat16)
    mine = jnp.concatenate([query_latent, own_rows[:, :, NOPE:]], axis=2).reshape(
        token_count, heads_dev * (LATENT + ROPE)
    )
    absorbed = lax.all_gather(mine, "ctx", axis=0, tiled=True).reshape(-1, heads_dev, LATENT + ROPE)
    highest, totals, head_out = local_attention(absorbed, latent_cache, cache_len[0], up_value)
    all_rows = absorbed.shape[0]
    got_out, got_high, got_total = (
        lax.all_to_all(
            head_out.reshape(all_rows, heads_dev * VDIM),
            "ctx",
            split_axis=0,
            concat_axis=0,
            tiled=True,
        ),
        lax.all_to_all(highest, "ctx", split_axis=0, concat_axis=0, tiled=True),
        lax.all_to_all(totals, "ctx", split_axis=0, concat_axis=0, tiled=True),
    )
    got_out = got_out.reshape(ctx_count, token_count, heads_dev, VDIM)
    got_high = got_high.reshape(ctx_count, token_count, heads_dev)
    got_total = got_total.reshape(ctx_count, token_count, heads_dev)
    overall = jnp.max(got_high, axis=0)
    factor = jnp.exp(got_high - overall[None])
    numerator = jnp.sum(got_out * factor[:, :, :, None], axis=0)
    denominator = jnp.sum(got_total * factor, axis=0)
    attention = (
        (numerator / denominator[:, :, None])
        .astype(jnp.bfloat16)
        .reshape(token_count, heads_dev * VDIM)
    )
    projected = jnp.dot(
        attention,
        lax.all_gather(o_weight, "ctx", axis=1, tiled=True),
        preferred_element_type=jnp.float32,
    )
    quarter = D // sub_count
    offset_cols = lax.axis_index("sub") * quarter
    hidden = residual.astype(jnp.float32) + lax.psum(projected.astype(jnp.bfloat16), "sub").astype(
        jnp.float32
    )
    inverse_rms = lax.rsqrt(jnp.mean(hidden * hidden, axis=1) + epsilon)
    normed = (hidden * inverse_rms[:, None] * norm_gain.astype(jnp.float32)).astype(jnp.bfloat16)
    hidden_part = lax.dynamic_slice_in_dim(hidden, offset_cols, quarter, 1)
    experts_dev = w_gate.shape[0]
    expert_total = experts_dev * ctx_count
    pair_count = token_count * TOP
    expert_ids = route_ids.reshape(pair_count)
    onehot = (expert_ids[:, None] == lax.broadcasted_iota(jnp.int32, (1, expert_total), 1)).astype(
        jnp.int32
    )
    earlier = jnp.cumsum(onehot, axis=0) - onehot
    slot_ids = jnp.sum(earlier * onehot, axis=1)
    targets = (expert_ids * CAP + slot_ids).reshape(token_count, TOP)
    matches = targets[:, :, None] == lax.broadcasted_iota(jnp.int32, (1, 1, expert_total * CAP), 2)
    select = jnp.sum(matches.astype(jnp.int32), axis=1).astype(jnp.bfloat16)
    outgoing = jnp.einsum("tj,td->jd", select, normed, preferred_element_type=jnp.float32).astype(
        jnp.bfloat16
    )
    outgoing = outgoing.reshape(ctx_count, experts_dev, CAP, D)
    received = lax.all_to_all(outgoing, "ctx", split_axis=0, concat_axis=0, tiled=True)
    gate_act = jnp.einsum("sekd,edf->sekf", received, w_gate, preferred_element_type=jnp.float32)
    up_act = jnp.einsum("sekd,edf->sekf", received, w_up, preferred_element_type=jnp.float32)
    gated_rows = (jax.nn.silu(gate_act) * up_act).astype(jnp.bfloat16)
    partial_out = jnp.einsum(
        "sekf,efd->sekd", gated_rows, w_down, preferred_element_type=jnp.float32
    )
    summed = lax.psum_scatter(
        partial_out.astype(jnp.bfloat16), "sub", scatter_dimension=3, tiled=True
    )
    back_rows = lax.all_to_all(summed, "ctx", split_axis=0, concat_axis=0, tiled=True)
    back_rows = back_rows.reshape(expert_total * CAP, quarter)
    mixing = jnp.sum(jnp.where(matches, route_weights[:, :, None], 0.0), axis=1)
    routed = jnp.dot(mixing, back_rows.astype(jnp.float32), precision=lax.Precision.HIGHEST)
    return (hidden_part + routed).astype(jnp.bfloat16)


LANES = 128
TILE = 256
CHUNKS = 1
MESH = pl.DeviceIdType.MESH
F32 = jnp.float32
BF16 = jnp.bfloat16
NT = (((1,), (1,)), ((), ()))


def fused_kernel(
    dims,
    q_hbm,
    res_hbm,
    ids_hbm,
    mix_hbm,
    len_hbm,
    cache_hbm,
    kv_hbm,
    o_hbm,
    gain_hbm,
    gate_hbm,
    up_hbm,
    down_hbm,
    out_ref,
    res_ref,
    ids_ref,
    mix_ref,
    len_ref,
    cache_ref,
    kv_ref,
    o_ref,
    gain_ref,
    q_all,
    res_all,
    comb_send,
    comb_all,
    ql_all,
    lat_send,
    lat_all,
    stat_all,
    att_all,
    proj_send,
    proj_all,
    hid_all,
    gain_rows,
    tokens,
    gate_sum,
    up_sum,
    mix_cols,
    gated,
    pair_send,
    pair_all,
    fin_send,
    fin_all,
    gate_buf,
    up_buf,
    down_buf,
    in_sem,
    w_sem,
    ctx_send,
    ctx_recv,
    comb_ssem,
    comb_rsem,
    sub_send,
    sub_recv,
    hid_ssem,
    hid_rsem,
    pair_ssem,
    pair_rsem,
    fin_ssem,
    fin_rsem,
):
    grp, ctx, sub, tok, heads, experts = dims
    me_g = lax.axis_index("grp")
    me_c = lax.axis_index("ctx")
    me_s = lax.axis_index("sub")
    span = ctx * tok
    rows = heads * span
    chunk = rows // CHUNKS
    chunk_heads = heads // CHUNKS
    quarter = o_ref.shape[1]
    hidden_units = gate_hbm.shape[1]

    barrier = pltpu.get_barrier_semaphore()

    def everyone():
        for dg in range(grp):
            for dc in range(ctx):
                for ds in range(sub):
                    if dg or dc or ds:
                        yield (
                            (dg * ctx + dc) * sub + ds,
                            lax.rem(me_g + dg, grp),
                            lax.rem(me_c + dc, ctx),
                            lax.rem(me_s + ds, sub),
                        )

    loads = [
        pltpu.make_async_copy(source, target, in_sem.at[i])
        for i, (source, target) in enumerate(
            (
                (q_hbm, q_all.at[me_c]),
                (kv_hbm, kv_ref),
                (res_hbm, res_ref),
                (ids_hbm, ids_ref),
                (mix_hbm, mix_ref),
                (len_hbm, len_ref),
                (cache_hbm, cache_ref),
                (o_hbm, o_ref),
                (gain_hbm, gain_ref),
            )
        )
    ]
    q_load, kv_load, res_load, ids_load, mix_load, len_load, cache_load, o_load, gain_load = loads
    for load in loads:
        load.start()

    for _, pg, pc, ps in everyone():
        pl.semaphore_signal(
            barrier,
            inc=1,
            device_id={"grp": pg, "ctx": pc, "sub": ps},
            device_id_type=MESH,
        )

    weight_loads = []
    for i, (source, target) in enumerate(
        ((gate_hbm, gate_buf), (up_hbm, up_buf), (down_hbm, down_buf))
    ):
        for e in range(experts):
            place = pl.ds(e * hidden_units, hidden_units)
            weight_loads.append(
                pltpu.make_async_copy(
                    source.at[me_g * experts + e], target.at[place], w_sem.at[e, i]
                )
            )
            weight_loads[-1].start(priority=1)
    tiles = experts * hidden_units // TILE

    def turn_tiles(buffer, loads, first=0, last=tiles):
        for load in loads:
            load.wait()

        def turn(t, carry):
            place = pl.ds(pl.multiple_of(t * TILE, TILE), TILE)
            for j in range(buffer.shape[1] // TILE):
                cols = slice(j * TILE, (j + 1) * TILE)
                buffer[place, cols] = buffer[place, cols].T
            return carry

        lax.fori_loop(first, last, turn, 0)

    upper = me_c // (ctx // 2)
    sends = []

    def far(i):
        low = ctx - 1 - i
        low = low - (me_c - low + ctx) // ctx
        high = i + (i - me_c + ctx) // ctx
        return low + upper * (high - low)

    far_first = [far(i) for i in range(ctx - 1)]
    near_first = far_first[::-1]

    def send(source, target, send_sem, recv_sem, **peer):
        copy = pltpu.make_async_remote_copy(
            src_ref=source,
            dst_ref=target,
            send_sem=send_sem,
            recv_sem=recv_sem,
            device_id=peer,
            device_id_type=MESH,
        )
        copy.start()
        sends.append(copy)

    def arrived(target, recv_sem):
        pltpu.make_async_remote_copy(
            src_ref=target,
            dst_ref=target,
            send_sem=sub_send.at[0],
            recv_sem=recv_sem,
            device_id={"ctx": far_first[0]},
            device_id_type=MESH,
        ).wait_recv()

    def ctx_copies(phase, source_of, target_of):
        for i, peer in enumerate(far_first):
            send(
                source_of(peer),
                target_of(me_c),
                ctx_send.at[phase, i],
                ctx_recv.at[phase, me_c],
                ctx=peer,
            )
        return [(target_of(peer), ctx_recv.at[phase, peer]) for peer in near_first]

    def finish(arrivals):
        for arrival in arrivals:
            arrived(*arrival)

    q_load.wait()
    pl.semaphore_wait(barrier, grp * ctx * sub - 1)

    q_copies = ctx_copies(0, lambda peer: q_all.at[me_c], lambda c: q_all.at[c])

    res_load.wait()
    piece = quarter // sub

    def own_piece(peer):
        return pl.ds(pl.multiple_of(peer * quarter + me_s * piece, piece), piece)

    early = ctx_copies(
        1, lambda peer: res_ref.at[:, own_piece(peer)], lambda c: res_all.at[c]
    )
    res_all[me_c] = res_ref[:, own_piece(me_c)]

    ids_load.wait()
    mix_load.wait()
    lane = lax.broadcasted_iota(jnp.int32, (tok, LANES), 1)
    ids, mixes = ids_ref[...], mix_ref[...]
    for c in range(ctx):
        for g in range(grp):
            first = (c * grp + g) * experts
            comb = jnp.zeros((tok, LANES), F32)
            for k in range(TOP):
                hit = (ids[:, k : k + 1] == lane + first) & (lane < experts)
                comb += jnp.where(hit, mixes[:, k : k + 1], 0.0)
            comb_send[g * ctx + c] = comb
    comb_all[me_g * ctx + me_c] = comb_send[me_g * ctx + me_c]
    me_gc = me_g * ctx + me_c
    for dg in range(grp):
        pg = lax.rem(me_g + dg, grp)
        for i, pc in enumerate(far_first if dg == 0 else far_first + [me_c]):
            send(
                comb_send.at[pg * ctx + pc],
                comb_all.at[me_gc],
                comb_ssem.at[dg * ctx + i],
                comb_rsem.at[me_gc],
                grp=pg,
                ctx=pc,
            )
            early.append((comb_all.at[pg * ctx + pc], comb_rsem.at[pg * ctx + pc]))

    kv_load.wait()
    finish(q_copies)
    per_head = NOPE + ROPE
    q_rows = q_all[...].astype(F32).reshape(span, heads * per_head)
    turned = [
        q_rows if h == 0 else pltpu.roll(q_rows, (heads - h) * per_head, 1) for h in range(heads)
    ]
    ql_copies = []
    for k in range(CHUNKS):
        for h in range(k * chunk_heads, (k + 1) * chunk_heads):
            nope = turned[h][:, :NOPE].astype(BF16)
            part = jnp.dot(nope, kv_ref[h, :NOPE, :], preferred_element_type=F32).astype(BF16)
            ql_all[me_c, h * span : (h + 1) * span, :] = part
        block = pl.ds(k * chunk, chunk)
        ql_copies.append(
            ctx_copies(2 + k, lambda peer: ql_all.at[me_c, block], lambda c: ql_all.at[c, block])
        )

    cache_load.wait()
    len_load.wait()
    position = lax.broadcasted_iota(jnp.int32, (1, cache_ref.shape[1]), 1)
    live = position < len_ref[0]
    rope_scores = []
    for k in range(CHUNKS):
        rope = jnp.concatenate(
            [
                turned[h][:, NOPE:per_head]
                for h in range(k * chunk_heads, (k + 1) * chunk_heads)
            ],
            axis=0,
        ).astype(BF16)
        rope_scores.append(jnp.dot(rope, cache_ref[LATENT:, :], preferred_element_type=F32))

    turn_tiles(gate_buf, weight_loads[:experts], 0, 2 * tiles // 3)
    lat_copies = []
    for k in range(CHUNKS):
        finish(ql_copies[k])
        part = slice(k * chunk, (k + 1) * chunk)
        lat_q = jnp.concatenate([ql_all[c, part, :] for c in range(ctx)], axis=1)
        scores = jnp.dot(lat_q, cache_ref[:LATENT, :], preferred_element_type=F32)
        scores = (scores + rope_scores[k]) * (NOPE + ROPE) ** (-0.5)
        scores = jnp.where(live, scores, -jnp.inf)
        highest = jnp.max(scores, axis=1, keepdims=True)
        weights = jnp.exp(scores - highest).astype(BF16)
        latent = lax.dot_general(
            weights, cache_ref[:LATENT, :], NT, preferred_element_type=F32
        ).astype(BF16)
        for c in range(ctx):
            lat_send[c, part, :] = latent[:, c * LANES : (c + 1) * LANES]
        block = pl.ds(k * chunk, chunk)
        copies = ctx_copies(
            2 + CHUNKS + k,
            lambda peer: lat_send.at[peer, block],
            lambda c: lat_all.at[c, block],
        )
        lat_all[me_c, part, :] = lat_send[me_c, part, :]
        totals = jnp.sum(weights.astype(F32), axis=1, keepdims=True)
        side = lax.broadcasted_iota(jnp.int32, (chunk, LANES), 1)
        stats = jnp.where(side < 4, highest, totals).T
        stat_all[me_c, k] = stats[0:8, :]
        copies += ctx_copies(
            2 + 2 * CHUNKS + k, lambda peer: stat_all.at[me_c, k], lambda c: stat_all.at[c, k]
        )
        lat_copies.append(copies)

    turn_tiles(gate_buf, [], 2 * tiles // 3)
    turn_tiles(up_buf, weight_loads[experts : 2 * experts], 0, tiles // 3)
    att_copies = []
    for k in range(CHUNKS):
        finish(lat_copies[k])
        part = slice(k * chunk, (k + 1) * chunk)
        highs = [stat_all[c, k, 0:1, :] for c in range(ctx)]
        overall = functools.reduce(jnp.maximum, highs)
        factors = [jnp.exp(high - overall) for high in highs]
        denominator = sum(f * stat_all[c, k, 4:5, :] for c, f in enumerate(factors))
        merged = jnp.zeros((chunk, LANES), F32)
        for c in range(ctx):
            scale = jnp.broadcast_to(factors[c] / denominator, (LANES, chunk)).T
            merged += lat_all[c, part, :].astype(F32) * scale
        merged = merged.astype(BF16)
        for j in range(chunk_heads):
            h = k * chunk_heads + j
            out = lax.dot_general(
                merged[j * span : (j + 1) * span, :],
                kv_ref[h, NOPE:, :],
                NT,
                preferred_element_type=F32,
            )
            att_all[me_c, k, :, j * VDIM : (j + 1) * VDIM] = out.astype(BF16)
        att_copies.append(
            ctx_copies(
                2 + 3 * CHUNKS + k, lambda peer: att_all.at[me_c, k], lambda c: att_all.at[c, k]
            )
        )

    turn_tiles(up_buf, [], tiles // 3)
    o_load.wait()
    width = chunk_heads * VDIM
    projected = jnp.zeros((span, quarter), F32)
    for k in range(CHUNKS):
        finish(att_copies[k])
        attention = sum(att_all[c, k].astype(F32) for c in range(ctx)).astype(BF16)
        projected += jnp.dot(
            attention, o_ref[k * width : (k + 1) * width, :], preferred_element_type=F32
        )
    for s in range(sub):
        proj_send[s] = projected[:, s * piece : (s + 1) * piece].astype(BF16)
    copies = []
    for d in range(1, sub):
        peer = lax.rem(me_s + d, sub)
        send(proj_send.at[peer], proj_all.at[me_s], sub_send.at[d], sub_recv.at[me_s], sub=peer)
        copies.append((proj_all.at[peer], sub_recv.at[peer]))
    proj_all[me_s] = proj_send[me_s]
    finish(early)
    gain_load.wait()
    gain_rows[...] = gain_ref[...].astype(F32)

    comb = comb_all[...].reshape(grp * span, LANES)
    comb_lane = lax.broadcasted_iota(jnp.int32, (grp * span, LANES), 1)
    columns = [
        jnp.sum(jnp.where(comb_lane == e, comb, 0.0), axis=1, keepdims=True)
        for e in range(experts)
    ]
    for t in range(experts * hidden_units // LANES):
        low, high = t * LANES // hidden_units, (t * LANES + LANES - 1) // hidden_units
        mix = jnp.broadcast_to(columns[low], (grp * span, LANES))
        if high > low:
            mix = jnp.where(comb_lane < high * hidden_units - t * LANES, mix, columns[high])
        mix_cols[:, t * LANES : (t + 1) * LANES] = mix

    residual = res_all[...].astype(F32).reshape(span, piece)
    finish(copies)
    me = (me_g * ctx + me_c) * sub + me_s
    hid_all[me] = (residual + sum(proj_all[s].astype(F32) for s in range(sub))).astype(BF16)
    def spread(pc, k):
        slot = (me_g * ctx + pc) * sub + me_s
        count = 0
        for dg in range(grp):
            for ds in range(sub):
                if dg or ds:
                    send(
                        hid_all.at[slot],
                        hid_all.at[slot],
                        hid_ssem.at[k * grp * sub + count],
                        hid_rsem.at[slot],
                        grp=lax.rem(me_g + dg, grp),
                        sub=lax.rem(me_s + ds, sub),
                    )
                    count += 1

    for i, pc in enumerate(far_first):
        send(
            hid_all.at[me],
            hid_all.at[me],
            hid_ssem.at[i * grp * sub + grp * sub - 1],
            hid_rsem.at[me],
            ctx=pc,
        )
    spread(me_c, 0)

    def relay(k):
        slot = (me_g * ctx + near_first[k - 1]) * sub + me_s
        arrived(hid_all.at[slot], hid_rsem.at[slot])
        spread(near_first[k - 1], k)

    for load in weight_loads[2 * experts :]:
        load.wait()
    squares = [jnp.zeros((span, piece), F32) for _ in range(grp)]
    for k in range(ctx):
        pc = me_c if k == 0 else near_first[k - 1]
        for dg in range(grp):
            for ds in range(sub):
                if dg or ds:
                    at = (lax.rem(me_g + dg, grp) * ctx + pc) * sub + lax.rem(me_s + ds, sub)
                    arrived(hid_all.at[at], hid_rsem.at[at])
        for g in range(grp):
            for t in range(sub):
                block = hid_all[(g * ctx + pc) * sub + t].astype(F32)
                squares[g] += block * block
                scaled = block * gain_rows[pl.ds(pc * sub + t, 1), :]
                tokens[k, g * span : (g + 1) * span, t * piece : (t + 1) * piece] = scaled.astype(
                    BF16
                )
        if k == ctx - 1:
            means = jnp.sum(jnp.concatenate(squares, axis=0), axis=1, keepdims=True) / (
                ctx * quarter
            )
            inverse_rms = lax.rsqrt(means + epsilon)
        halves = quarter // TILE
        cols = [
            pl.ds(pl.multiple_of(pc * quarter + n * TILE, TILE), TILE) for n in range(halves)
        ]
        for t in range(tiles):
            if k == 0:
                for ahead in range(1, ctx):
                    if t == (ahead - 1) * tiles // ctx:
                        relay(ahead)
            tile = slice(t * TILE, (t + 1) * TILE)

            def product(buffer):
                return sum(
                    jnp.dot(
                        tokens[k, :, n * TILE : (n + 1) * TILE],
                        buffer[tile, cols[n]],
                        preferred_element_type=F32,
                    )
                    for n in range(halves)
                )

            gate_act, up_act = product(gate_buf), product(up_buf)
            if k > 0:
                gate_act += gate_sum[:, tile]
                up_act += up_sum[:, tile]
            if k < ctx - 1:
                gate_sum[:, tile] = gate_act
                up_sum[:, tile] = up_act
            else:
                gate_act *= inverse_rms
                both = gate_act / (1.0 + jnp.exp(-gate_act)) * (up_act * inverse_rms)
                gated[:, tile] = (both * mix_cols[:, tile]).astype(BF16)

    pairs = sub // 2
    me_p, side = me_s // 2, lax.rem(me_s, 2)

    def down(s):
        cols = pl.ds(pl.multiple_of(s * quarter, quarter), quarter)
        return jnp.dot(gated[...], down_buf[:, cols], preferred_element_type=F32)

    turns = [lax.rem(me_p + dp, pairs) for dp in range(1, pairs)] + [me_p]
    for n, pp in enumerate(turns):
        pair_send[n] = down(2 * pp + 1 - side).astype(BF16)
        send(
            pair_send.at[n],
            pair_all.at[pp],
            pair_ssem.at[n],
            pair_rsem.at[pp],
            sub=2 * me_p + 1 - side,
        )
    arrivals = []
    me_half = me_gc * pairs + me_p
    for n, pp in enumerate(turns):
        block = down(2 * pp + side)
        arrived(pair_all.at[pp], pair_rsem.at[pp])
        block = (block + pair_all[pp].astype(F32)).astype(BF16)
        for i in range(grp * ctx):
            fin_send[n, i] = block[i * tok : (i + 1) * tok, :]
        count = 0
        for pc in far_first + [me_c]:
            for dg in range(grp):
                pg = lax.rem(me_g + dg, grp)
                if pc is me_c and dg == 0 and n == pairs - 1:
                    fin_all[me_half] = fin_send[n, me_gc]
                    continue
                send(
                    fin_send.at[n, pg * ctx + pc],
                    fin_all.at[me_half],
                    fin_ssem.at[n * grp * ctx + count],
                    fin_rsem.at[me_half],
                    grp=pg,
                    ctx=pc,
                    sub=2 * pp + side,
                )
                count += 1
                at = (pg * ctx + pc) * pairs + pp
                arrivals.append((fin_all.at[at], fin_rsem.at[at]))
    hidden = jnp.concatenate(
        [hid_all[(me_g * ctx + me_s) * sub + t].astype(F32) for t in range(sub)],
        axis=1,
    )
    mine = jnp.zeros((tok, quarter), F32)
    for c in range(ctx):
        mine += jnp.where(me_c == c, hidden[c * tok : (c + 1) * tok, :], 0.0)
    finish(arrivals)
    routed = sum(fin_all[i].astype(F32) for i in range(grp * ctx * pairs))
    out_ref[...] = (mine + routed).astype(out_ref.dtype)
    for copy in sends:
        copy.wait_send()


def fused_body(
    queries,
    latent_cache,
    cache_len,
    kv_up,
    o_weight,
    residual,
    norm_gain,
    route_ids,
    route_weights,
    w_gate,
    w_up,
    w_down,
):
    grp, ctx, sub = lax.axis_size("grp"), lax.axis_size("ctx"), lax.axis_size("sub")
    heads, tok, experts = kv_up.shape[0], queries.shape[0], w_gate.shape[0] // grp
    span, rows, quarter = ctx * tok, heads * ctx * tok, o_weight.shape[1]
    width, piece, everyone = residual.shape[1], quarter // sub, grp * ctx * sub
    w_gate, w_up = jnp.swapaxes(w_gate, 1, 2), jnp.swapaxes(w_up, 1, 2)
    units = experts * w_gate.shape[1]
    cache = latent_cache.T
    gain = norm_gain.reshape(width // LANES, LANES)
    hbm = pl.BlockSpec(memory_space=pl.ANY)
    dma = pltpu.SemaphoreType.DMA
    out = pl.pallas_call(
        functools.partial(fused_kernel, (grp, ctx, sub, tok, heads, experts)),
        out_shape=jax.ShapeDtypeStruct((tok, width // sub), F32),
        in_specs=[hbm] * 12,
        out_specs=pl.BlockSpec(memory_space=pltpu.VMEM),
        scratch_shapes=[
            pltpu.VMEM(residual.shape, BF16),
            pltpu.VMEM(route_ids.shape, jnp.int32),
            pltpu.VMEM(route_weights.shape, F32),
            pltpu.SMEM(cache_len.shape, jnp.int32),
            pltpu.VMEM(cache.shape, BF16),
            pltpu.VMEM(kv_up.shape, BF16),
            pltpu.VMEM(o_weight.shape, BF16),
            pltpu.VMEM(gain.shape, BF16),
            pltpu.VMEM((ctx,) + queries.shape, BF16),
            pltpu.VMEM((ctx, tok, piece), BF16),
            pltpu.VMEM((grp * ctx, tok, LANES), F32),
            pltpu.VMEM((grp * ctx, tok, LANES), F32),
            pltpu.VMEM((ctx, rows, LANES), BF16),
            pltpu.VMEM((ctx, rows, LANES), BF16),
            pltpu.VMEM((ctx, rows, LANES), BF16),
            pltpu.VMEM((ctx, CHUNKS, 8, rows // CHUNKS), F32),
            pltpu.VMEM((ctx, CHUNKS, span, heads * VDIM // CHUNKS), BF16),
            pltpu.VMEM((sub, span, piece), BF16),
            pltpu.VMEM((sub, span, piece), BF16),
            pltpu.VMEM((everyone, span, piece), BF16),
            pltpu.VMEM(gain.shape, F32),
            pltpu.VMEM((ctx, grp * span, quarter), BF16),
            pltpu.VMEM((grp * span, units), F32),
            pltpu.VMEM((grp * span, units), F32),
            pltpu.VMEM((grp * span, units), F32),
            pltpu.VMEM((grp * span, units), BF16),
            pltpu.VMEM((sub // 2, grp * span, quarter), BF16),
            pltpu.VMEM((sub // 2, grp * span, quarter), BF16),
            pltpu.VMEM((sub // 2, grp * ctx, tok, quarter), BF16),
            pltpu.VMEM((everyone // 2, tok, quarter), BF16),
            pltpu.VMEM((units, width), BF16),
            pltpu.VMEM((units, width), BF16),
            pltpu.VMEM((units, width), BF16),
            dma((9,)),
            dma((experts, 3)),
            dma((2 + 4 * CHUNKS, ctx)),
            dma((2 + 4 * CHUNKS, ctx)),
            dma((grp * ctx,)),
            dma((grp * ctx,)),
            dma((sub,)),
            dma((sub,)),
            dma((everyone,)),
            dma((everyone,)),
            dma((sub // 2,)),
            dma((sub // 2,)),
            dma((everyone // 2,)),
            dma((everyone // 2,)),
        ],
        compiler_params=pltpu.CompilerParams(
            collective_id=0, has_side_effects=True, vmem_limit_bytes=46 * 1024 * 1024
        ),
    )(
        *(
            operand
            if operand is cache_len
            else pltpu.with_memory_space_constraint(operand, pltpu.HBM)
            for operand in (
                queries,
                residual,
                route_ids,
                route_weights,
                cache_len,
                cache,
                kv_up,
                o_weight,
                gain,
                w_gate,
                w_up,
                w_down,
            )
        )
    )
    return out.astype(BF16)


def choose_body(*args):
    kv_up, o_weight, w_gate = args[3], args[4], args[9]
    grp, ctx, sub = lax.axis_size("grp"), lax.axis_size("ctx"), lax.axis_size("sub")
    tok, experts = args[0].shape[0], w_gate.shape[0]
    units = experts // grp * w_gate.shape[2]
    fits = (
        ctx == sub
        and ctx % 2 == 0
        and kv_up.shape[2] == LANES
        and o_weight.shape[1] == sub * LANES
        and kv_up.shape[0] * ctx * tok == LANES
        and experts % grp == 0
        and experts <= LANES
        and w_gate.shape[2] % 16 == 0
        and units % TILE == 0
        and o_weight.shape[1] % TILE == 0
        and units * w_gate.shape[1] * 6 <= 40 * 1024 * 1024
        and tok % 8 == 0
    )
    return fused_body(*args) if fits else body(*args)


def solution(mesh):
    in_specs = (
        P(("grp", "ctx"), "sub"),
        P(("grp", "ctx"), None),
        P(("grp", "ctx")),
        P(("grp", "sub"), None, "ctx"),
        P("sub", "ctx"),
        P(("grp", "ctx"), None),
        P(),
        P(("grp", "ctx"), None),
        P(("grp", "ctx"), None),
        P("ctx", None, "sub"),
        P("ctx", None, "sub"),
        P("ctx", "sub", None),
    )
    out_specs = P(("grp", "ctx"), "sub")
    return jax.shard_map(choose_body, mesh=mesh, in_specs=in_specs, out_specs=out_specs, check_vma=False)
```

```python
import functools

import jax
import jax.numpy as jnp
from jax import lax
from jax.experimental import pallas as pl
from jax.experimental.pallas import tpu as pltpu
from jax.sharding import PartitionSpec as P

D = 2048
NOPE = 128
ROPE = 64
VDIM = 128
LATENT = 512
TOP = 6
CAP = 2


epsilon = 1e-06


def local_attention(absorbed, cache_rows, length, up_value):
    scores = jnp.einsum("qhc,kc->qhk", absorbed, cache_rows, preferred_element_type=jnp.float32) * (
        NOPE + ROPE
    ) ** (-0.5)
    live_mask = lax.broadcasted_iota(jnp.int32, (cache_rows.shape[0],), 0) < length
    scores = jnp.where(live_mask[None, None, :], scores, -jnp.inf)
    highest = jnp.max(scores, axis=2)
    weights = jnp.exp(scores - highest[:, :, None]).astype(jnp.bfloat16)
    totals = jnp.sum(weights, axis=2, dtype=jnp.float32)
    latent_out = jnp.einsum(
        "qhk,kl->qhl", weights, cache_rows[:, :LATENT], preferred_element_type=jnp.float32
    ).astype(jnp.bfloat16)
    head_out = jnp.einsum("qhl,hvl->qhv", latent_out, up_value, preferred_element_type=jnp.float32)
    return (highest, totals, head_out)


def body(
    queries,
    latent_cache,
    cache_len,
    kv_up,
    o_weight,
    residual,
    norm_gain,
    route_ids,
    route_weights,
    w_gate,
    w_up,
    w_down,
):
    ctx_count = lax.axis_size("ctx")
    sub_count = lax.axis_size("sub")
    heads_dev = kv_up.shape[0]
    token_count = queries.shape[0]
    up_full = lax.all_gather(kv_up, "ctx", axis=2, tiled=True)
    up_key = up_full[:, :NOPE, :]
    up_value = up_full[:, NOPE:, :]
    own_rows = queries.reshape(token_count, heads_dev, NOPE + ROPE)
    query_latent = jnp.einsum(
        "qhn,hnl->qhl", own_rows[:, :, :NOPE], up_key, preferred_element_type=jnp.float32
    ).astype(jnp.bfloat16)
    mine = jnp.concatenate([query_latent, own_rows[:, :, NOPE:]], axis=2).reshape(
        token_count, heads_dev * (LATENT + ROPE)
    )
    absorbed = lax.all_gather(mine, "ctx", axis=0, tiled=True).reshape(-1, heads_dev, LATENT + ROPE)
    highest, totals, head_out = local_attention(absorbed, latent_cache, cache_len[0], up_value)
    all_rows = absorbed.shape[0]
    got_out, got_high, got_total = (
        lax.all_to_all(
            head_out.reshape(all_rows, heads_dev * VDIM),
            "ctx",
            split_axis=0,
            concat_axis=0,
            tiled=True,
        ),
        lax.all_to_all(highest, "ctx", split_axis=0, concat_axis=0, tiled=True),
        lax.all_to_all(totals, "ctx", split_axis=0, concat_axis=0, tiled=True),
    )
    got_out = got_out.reshape(ctx_count, token_count, heads_dev, VDIM)
    got_high = got_high.reshape(ctx_count, token_count, heads_dev)
    got_total = got_total.reshape(ctx_count, token_count, heads_dev)
    overall = jnp.max(got_high, axis=0)
    factor = jnp.exp(got_high - overall[None])
    numerator = jnp.sum(got_out * factor[:, :, :, None], axis=0)
    denominator = jnp.sum(got_total * factor, axis=0)
    attention = (
        (numerator / denominator[:, :, None])
        .astype(jnp.bfloat16)
        .reshape(token_count, heads_dev * VDIM)
    )
    projected = jnp.dot(
        attention,
        lax.all_gather(o_weight, "ctx", axis=1, tiled=True),
        preferred_element_type=jnp.float32,
    )
    quarter = D // sub_count
    offset_cols = lax.axis_index("sub") * quarter
    hidden = residual.astype(jnp.float32) + lax.psum(projected.astype(jnp.bfloat16), "sub").astype(
        jnp.float32
    )
    inverse_rms = lax.rsqrt(jnp.mean(hidden * hidden, axis=1) + epsilon)
    normed = (hidden * inverse_rms[:, None] * norm_gain.astype(jnp.float32)).astype(jnp.bfloat16)
    hidden_part = lax.dynamic_slice_in_dim(hidden, offset_cols, quarter, 1)
    experts_dev = w_gate.shape[0]
    expert_total = experts_dev * ctx_count
    pair_count = token_count * TOP
    expert_ids = route_ids.reshape(pair_count)
    onehot = (expert_ids[:, None] == lax.broadcasted_iota(jnp.int32, (1, expert_total), 1)).astype(
        jnp.int32
    )
    earlier = jnp.cumsum(onehot, axis=0) - onehot
    slot_ids = jnp.sum(earlier * onehot, axis=1)
    targets = (expert_ids * CAP + slot_ids).reshape(token_count, TOP)
    matches = targets[:, :, None] == lax.broadcasted_iota(jnp.int32, (1, 1, expert_total * CAP), 2)
    select = jnp.sum(matches.astype(jnp.int32), axis=1).astype(jnp.bfloat16)
    outgoing = jnp.einsum("tj,td->jd", select, normed, preferred_element_type=jnp.float32).astype(
        jnp.bfloat16
    )
    outgoing = outgoing.reshape(ctx_count, experts_dev, CAP, D)
    received = lax.all_to_all(outgoing, "ctx", split_axis=0, concat_axis=0, tiled=True)
    gate_act = jnp.einsum("sekd,edf->sekf", received, w_gate, preferred_element_type=jnp.float32)
    up_act = jnp.einsum("sekd,edf->sekf", received, w_up, preferred_element_type=jnp.float32)
    gated_rows = (jax.nn.silu(gate_act) * up_act).astype(jnp.bfloat16)
    partial_out = jnp.einsum(
        "sekf,efd->sekd", gated_rows, w_down, preferred_element_type=jnp.float32
    )
    summed = lax.psum_scatter(
        partial_out.astype(jnp.bfloat16), "sub", scatter_dimension=3, tiled=True
    )
    back_rows = lax.all_to_all(summed, "ctx", split_axis=0, concat_axis=0, tiled=True)
    back_rows = back_rows.reshape(expert_total * CAP, quarter)
    mixing = jnp.sum(jnp.where(matches, route_weights[:, :, None], 0.0), axis=1)
    routed = jnp.dot(mixing, back_rows.astype(jnp.float32), precision=lax.Precision.HIGHEST)
    return (hidden_part + routed).astype(jnp.bfloat16)


LANES = 128
TILE = 256
CHUNKS = 1
MESH = pl.DeviceIdType.MESH
F32 = jnp.float32
BF16 = jnp.bfloat16
NT = (((1,), (1,)), ((), ()))


def fused_kernel(
    dims,
    q_hbm,
    res_hbm,
    ids_hbm,
    mix_hbm,
    len_hbm,
    cache_hbm,
    kv_hbm,
    o_hbm,
    gain_hbm,
    gate_hbm,
    up_hbm,
    down_hbm,
    out_ref,
    res_ref,
    ids_ref,
    mix_ref,
    len_ref,
    cache_ref,
    kv_ref,
    o_ref,
    gain_ref,
    q_all,
    res_all,
    comb_send,
    comb_all,
    ql_all,
    lat_send,
    lat_all,
    stat_all,
    att_all,
    proj_send,
    proj_all,
    hid_all,
    gain_rows,
    tokens,
    gate_sum,
    up_sum,
    mix_cols,
    gated,
    pair_send,
    pair_all,
    own_sum,
    fin_send,
    fin_all,
    gate_buf,
    up_buf,
    down_buf,
    in_sem,
    w_sem,
    ctx_send,
    ctx_recv,
    comb_ssem,
    comb_rsem,
    sub_send,
    sub_recv,
    hid_ssem,
    hid_rsem,
    pair_ssem,
    pair_rsem,
    fin_ssem,
    fin_rsem,
):
    grp, ctx, sub, tok, heads, experts = dims
    me_g = lax.axis_index("grp")
    me_c = lax.axis_index("ctx")
    me_s = lax.axis_index("sub")
    span = ctx * tok
    rows = heads * span
    chunk = rows // CHUNKS
    chunk_heads = heads // CHUNKS
    quarter = o_ref.shape[1]
    hidden_units = gate_hbm.shape[1]

    barrier = pltpu.get_barrier_semaphore()

    def everyone():
        for dg in range(grp):
            for dc in range(ctx):
                for ds in range(sub):
                    if dg or dc or ds:
                        yield (
                            (dg * ctx + dc) * sub + ds,
                            lax.rem(me_g + dg, grp),
                            lax.rem(me_c + dc, ctx),
                            lax.rem(me_s + ds, sub),
                        )

    loads = [
        pltpu.make_async_copy(source, target, in_sem.at[i])
        for i, (source, target) in enumerate(
            (
                (q_hbm, q_all.at[me_c]),
                (kv_hbm, kv_ref),
                (res_hbm, res_ref),
                (ids_hbm, ids_ref),
                (mix_hbm, mix_ref),
                (len_hbm, len_ref),
                (cache_hbm, cache_ref),
                (o_hbm, o_ref),
                (gain_hbm, gain_ref),
            )
        )
    ]
    q_load, kv_load, res_load, ids_load, mix_load, len_load, cache_load, o_load, gain_load = loads
    for load in loads:
        load.start()

    for _, pg, pc, ps in everyone():
        pl.semaphore_signal(
            barrier,
            inc=1,
            device_id={"grp": pg, "ctx": pc, "sub": ps},
            device_id_type=MESH,
        )

    weight_loads = []
    for i, (source, target) in enumerate(
        ((gate_hbm, gate_buf), (up_hbm, up_buf), (down_hbm, down_buf))
    ):
        for e in range(experts):
            place = pl.ds(e * hidden_units, hidden_units)
            weight_loads.append(
                pltpu.make_async_copy(
                    source.at[me_g * experts + e], target.at[place], w_sem.at[e, i]
                )
            )
            weight_loads[-1].start(priority=1)
    tiles = experts * hidden_units // TILE

    def turn_tiles(buffer, loads, first=0, last=tiles):
        for load in loads:
            load.wait()

        def turn(t, carry):
            place = pl.ds(pl.multiple_of(t * TILE, TILE), TILE)
            for j in range(buffer.shape[1] // TILE):
                cols = slice(j * TILE, (j + 1) * TILE)
                buffer[place, cols] = buffer[place, cols].T
            return carry

        lax.fori_loop(first, last, turn, 0)

    upper = me_c // (ctx // 2)
    sends = []

    def far(i):
        low = ctx - 1 - i
        low = low - (me_c - low + ctx) // ctx
        high = i + (i - me_c + ctx) // ctx
        return low + upper * (high - low)

    far_first = [far(i) for i in range(ctx - 1)]
    near_first = far_first[::-1]

    def send(source, target, send_sem, recv_sem, **peer):
        copy = pltpu.make_async_remote_copy(
            src_ref=source,
            dst_ref=target,
            send_sem=send_sem,
            recv_sem=recv_sem,
            device_id=peer,
            device_id_type=MESH,
        )
        copy.start()
        sends.append(copy)

    def arrived(target, recv_sem):
        pltpu.make_async_remote_copy(
            src_ref=target,
            dst_ref=target,
            send_sem=sub_send.at[0],
            recv_sem=recv_sem,
            device_id={"ctx": far_first[0]},
            device_id_type=MESH,
        ).wait_recv()

    def ctx_copies(phase, source_of, target_of):
        for i, peer in enumerate(far_first):
            send(
                source_of(peer),
                target_of(me_c),
                ctx_send.at[phase, i],
                ctx_recv.at[phase, me_c],
                ctx=peer,
            )
        return [(target_of(peer), ctx_recv.at[phase, peer]) for peer in near_first]

    def finish(arrivals):
        for arrival in arrivals:
            arrived(*arrival)

    q_load.wait()
    pl.semaphore_wait(barrier, grp * ctx * sub - 1)

    q_copies = ctx_copies(0, lambda peer: q_all.at[me_c], lambda c: q_all.at[c])

    res_load.wait()
    piece = quarter // sub

    def own_piece(peer):
        return pl.ds(pl.multiple_of(peer * quarter + me_s * piece, piece), piece)

    early = ctx_copies(
        1, lambda peer: res_ref.at[:, own_piece(peer)], lambda c: res_all.at[c]
    )
    res_all[me_c] = res_ref[:, own_piece(me_c)]

    ids_load.wait()
    mix_load.wait()
    lane = lax.broadcasted_iota(jnp.int32, (tok, LANES), 1)
    ids, mixes = ids_ref[...], mix_ref[...]
    for c in range(ctx):
        for g in range(grp):
            first = (c * grp + g) * experts
            comb = jnp.zeros((tok, LANES), F32)
            for k in range(TOP):
                hit = (ids[:, k : k + 1] == lane + first) & (lane < experts)
                comb += jnp.where(hit, mixes[:, k : k + 1], 0.0)
            comb_send[g * ctx + c] = comb
    comb_all[me_g * ctx + me_c] = comb_send[me_g * ctx + me_c]
    me_gc = me_g * ctx + me_c
    for dg in range(grp):
        pg = lax.rem(me_g + dg, grp)
        for i, pc in enumerate(far_first if dg == 0 else far_first + [me_c]):
            send(
                comb_send.at[pg * ctx + pc],
                comb_all.at[me_gc],
                comb_ssem.at[dg * ctx + i],
                comb_rsem.at[me_gc],
                grp=pg,
                ctx=pc,
            )
            early.append((comb_all.at[pg * ctx + pc], comb_rsem.at[pg * ctx + pc]))

    kv_load.wait()
    finish(q_copies)
    per_head = NOPE + ROPE
    q_rows = q_all[...].astype(F32).reshape(span, heads * per_head)
    turned = [
        q_rows if h == 0 else pltpu.roll(q_rows, (heads - h) * per_head, 1) for h in range(heads)
    ]
    ql_copies = []
    for k in range(CHUNKS):
        for h in range(k * chunk_heads, (k + 1) * chunk_heads):
            nope = turned[h][:, :NOPE].astype(BF16)
            part = jnp.dot(nope, kv_ref[h, :NOPE, :], preferred_element_type=F32).astype(BF16)
            ql_all[me_c, h * span : (h + 1) * span, :] = part
        block = pl.ds(k * chunk, chunk)
        ql_copies.append(
            ctx_copies(2 + k, lambda peer: ql_all.at[me_c, block], lambda c: ql_all.at[c, block])
        )

    cache_load.wait()
    len_load.wait()
    position = lax.broadcasted_iota(jnp.int32, (1, cache_ref.shape[1]), 1)
    live = position < len_ref[0]
    rope_scores = []
    for k in range(CHUNKS):
        rope = jnp.concatenate(
            [
                turned[h][:, NOPE:per_head]
                for h in range(k * chunk_heads, (k + 1) * chunk_heads)
            ],
            axis=0,
        ).astype(BF16)
        rope_scores.append(jnp.dot(rope, cache_ref[LATENT:, :], preferred_element_type=F32))

    turn_tiles(gate_buf, weight_loads[:experts], 0, 2 * tiles // 3)
    lat_copies = []
    for k in range(CHUNKS):
        finish(ql_copies[k])
        part = slice(k * chunk, (k + 1) * chunk)
        lat_q = jnp.concatenate([ql_all[c, part, :] for c in range(ctx)], axis=1)
        scores = jnp.dot(lat_q, cache_ref[:LATENT, :], preferred_element_type=F32)
        scores = (scores + rope_scores[k]) * (NOPE + ROPE) ** (-0.5)
        scores = jnp.where(live, scores, -jnp.inf)
        highest = jnp.max(scores, axis=1, keepdims=True)
        weights = jnp.exp(scores - highest).astype(BF16)
        latent = lax.dot_general(
            weights, cache_ref[:LATENT, :], NT, preferred_element_type=F32
        ).astype(BF16)
        for c in range(ctx):
            lat_send[c, part, :] = latent[:, c * LANES : (c + 1) * LANES]
        block = pl.ds(k * chunk, chunk)
        copies = ctx_copies(
            2 + CHUNKS + k,
            lambda peer: lat_send.at[peer, block],
            lambda c: lat_all.at[c, block],
        )
        lat_all[me_c, part, :] = lat_send[me_c, part, :]
        totals = jnp.sum(weights.astype(F32), axis=1, keepdims=True)
        side = lax.broadcasted_iota(jnp.int32, (chunk, LANES), 1)
        stats = jnp.where(side < 4, highest, totals).T
        stat_all[me_c, k] = stats[0:8, :]
        copies += ctx_copies(
            2 + 2 * CHUNKS + k, lambda peer: stat_all.at[me_c, k], lambda c: stat_all.at[c, k]
        )
        lat_copies.append(copies)

    turn_tiles(gate_buf, [], 2 * tiles // 3)
    turn_tiles(up_buf, weight_loads[experts : 2 * experts], 0, tiles // 3)
    att_copies = []
    for k in range(CHUNKS):
        finish(lat_copies[k])
        part = slice(k * chunk, (k + 1) * chunk)
        highs = [stat_all[c, k, 0:1, :] for c in range(ctx)]
        overall = functools.reduce(jnp.maximum, highs)
        factors = [jnp.exp(high - overall) for high in highs]
        denominator = sum(f * stat_all[c, k, 4:5, :] for c, f in enumerate(factors))
        merged = jnp.zeros((chunk, LANES), F32)
        for c in range(ctx):
            scale = jnp.broadcast_to(factors[c] / denominator, (LANES, chunk)).T
            merged += lat_all[c, part, :].astype(F32) * scale
        merged = merged.astype(BF16)
        for j in range(chunk_heads):
            h = k * chunk_heads + j
            out = lax.dot_general(
                merged[j * span : (j + 1) * span, :],
                kv_ref[h, NOPE:, :],
                NT,
                preferred_element_type=F32,
            )
            att_all[me_c, k, :, j * VDIM : (j + 1) * VDIM] = out.astype(BF16)
        att_copies.append(
            ctx_copies(
                2 + 3 * CHUNKS + k, lambda peer: att_all.at[me_c, k], lambda c: att_all.at[c, k]
            )
        )

    turn_tiles(up_buf, [], tiles // 3)
    o_load.wait()
    width = chunk_heads * VDIM
    projected = jnp.zeros((span, quarter), F32)
    for k in range(CHUNKS):
        finish(att_copies[k])
        attention = sum(att_all[c, k].astype(F32) for c in range(ctx)).astype(BF16)
        projected += jnp.dot(
            attention, o_ref[k * width : (k + 1) * width, :], preferred_element_type=F32
        )
    for s in range(sub):
        proj_send[s] = projected[:, s * piece : (s + 1) * piece].astype(BF16)
    copies = []
    for d in range(1, sub):
        peer = lax.rem(me_s + d, sub)
        send(proj_send.at[peer], proj_all.at[me_s], sub_send.at[d], sub_recv.at[me_s], sub=peer)
        copies.append((proj_all.at[peer], sub_recv.at[peer]))
    proj_all[me_s] = proj_send[me_s]
    finish(early)
    gain_load.wait()
    gain_rows[...] = gain_ref[...].astype(F32)

    comb = comb_all[...].reshape(grp * span, LANES)
    comb_lane = lax.broadcasted_iota(jnp.int32, (grp * span, LANES), 1)
    columns = [
        jnp.sum(jnp.where(comb_lane == e, comb, 0.0), axis=1, keepdims=True)
        for e in range(experts)
    ]
    for t in range(experts * hidden_units // LANES):
        low, high = t * LANES // hidden_units, (t * LANES + LANES - 1) // hidden_units
        mix = jnp.broadcast_to(columns[low], (grp * span, LANES))
        if high > low:
            mix = jnp.where(comb_lane < high * hidden_units - t * LANES, mix, columns[high])
        mix_cols[:, t * LANES : (t + 1) * LANES] = mix

    residual = res_all[...].astype(F32).reshape(span, piece)
    finish(copies)
    me = (me_g * ctx + me_c) * sub + me_s
    hid_all[me] = (residual + sum(proj_all[s].astype(F32) for s in range(sub))).astype(BF16)
    def spread(pc, k):
        slot = (me_g * ctx + pc) * sub + me_s
        count = 0
        for dg in range(grp):
            for ds in range(sub):
                if dg or ds:
                    send(
                        hid_all.at[slot],
                        hid_all.at[slot],
                        hid_ssem.at[k * grp * sub + count],
                        hid_rsem.at[slot],
                        grp=lax.rem(me_g + dg, grp),
                        sub=lax.rem(me_s + ds, sub),
                    )
                    count += 1

    for i, pc in enumerate(far_first):
        send(
            hid_all.at[me],
            hid_all.at[me],
            hid_ssem.at[i * grp * sub + grp * sub - 1],
            hid_rsem.at[me],
            ctx=pc,
        )
    spread(me_c, 0)

    def relay(k):
        slot = (me_g * ctx + near_first[k - 1]) * sub + me_s
        arrived(hid_all.at[slot], hid_rsem.at[slot])
        spread(near_first[k - 1], k)

    for load in weight_loads[2 * experts :]:
        load.wait()
    squares = [jnp.zeros((span, piece), F32) for _ in range(grp)]
    for k in range(ctx):
        pc = me_c if k == 0 else near_first[k - 1]
        for dg in range(grp):
            for ds in range(sub):
                if dg or ds:
                    at = (lax.rem(me_g + dg, grp) * ctx + pc) * sub + lax.rem(me_s + ds, sub)
                    arrived(hid_all.at[at], hid_rsem.at[at])
        for g in range(grp):
            for t in range(sub):
                block = hid_all[(g * ctx + pc) * sub + t].astype(F32)
                squares[g] += block * block
                scaled = block * gain_rows[pl.ds(pc * sub + t, 1), :]
                tokens[k, g * span : (g + 1) * span, t * piece : (t + 1) * piece] = scaled.astype(
                    BF16
                )
        if k == ctx - 1:
            means = jnp.sum(jnp.concatenate(squares, axis=0), axis=1, keepdims=True) / (
                ctx * quarter
            )
            inverse_rms = lax.rsqrt(means + epsilon)
        halves = quarter // TILE
        cols = [
            pl.ds(pl.multiple_of(pc * quarter + n * TILE, TILE), TILE) for n in range(halves)
        ]
        for t in range(tiles):
            if k == 0:
                for ahead in range(1, ctx):
                    if t == (ahead - 1) * tiles // ctx:
                        relay(ahead)
            tile = slice(t * TILE, (t + 1) * TILE)

            def product(buffer):
                return sum(
                    jnp.dot(
                        tokens[k, :, n * TILE : (n + 1) * TILE],
                        buffer[tile, cols[n]],
                        preferred_element_type=F32,
                    )
                    for n in range(halves)
                )

            gate_act, up_act = product(gate_buf), product(up_buf)
            if k > 0:
                gate_act += gate_sum[:, tile]
                up_act += up_sum[:, tile]
            if k < ctx - 1:
                gate_sum[:, tile] = gate_act
                up_sum[:, tile] = up_act
            else:
                gate_act *= inverse_rms
                both = gate_act / (1.0 + jnp.exp(-gate_act)) * (up_act * inverse_rms)
                gated[:, tile] = (both * mix_cols[:, tile]).astype(BF16)

    pairs = sub // 2
    me_p, side = me_s // 2, lax.rem(me_s, 2)

    def down(s):
        cols = pl.ds(pl.multiple_of(s * quarter, quarter), quarter)
        return jnp.dot(gated[...], down_buf[:, cols], preferred_element_type=F32)

    turns = [lax.rem(me_p + dp, pairs) for dp in range(1, pairs)] + [me_p]
    for n, pp in enumerate(turns):
        pair_send[n] = down(2 * pp + 1 - side).astype(BF16)
        send(
            pair_send.at[n],
            pair_all.at[pp],
            pair_ssem.at[n],
            pair_rsem.at[pp],
            sub=2 * me_p + 1 - side,
        )
    arrivals = []
    me_half = me_gc * pairs + me_p
    for n, pp in enumerate(turns):
        own_sum[n] = down(2 * pp + side)
        arrived(pair_all.at[pp], pair_rsem.at[pp])
        block = (own_sum[n] + pair_all[pp].astype(F32)).astype(BF16)
        for i in range(grp * ctx):
            fin_send[n, i] = block[i * tok : (i + 1) * tok, :]
        count = 0
        for pc in far_first + [me_c]:
            for dg in range(grp):
                pg = lax.rem(me_g + dg, grp)
                if pc is me_c and dg == 0 and n == pairs - 1:
                    fin_all[me_half] = fin_send[n, me_gc]
                    continue
                send(
                    fin_send.at[n, pg * ctx + pc],
                    fin_all.at[me_half],
                    fin_ssem.at[n * grp * ctx + count],
                    fin_rsem.at[me_half],
                    grp=pg,
                    ctx=pc,
                    sub=2 * pp + side,
                )
                count += 1
                at = (pg * ctx + pc) * pairs + pp
                arrivals.append((fin_all.at[at], fin_rsem.at[at]))
    hidden = jnp.concatenate(
        [hid_all[(me_g * ctx + me_s) * sub + t].astype(F32) for t in range(sub)],
        axis=1,
    )
    mine = jnp.zeros((tok, quarter), F32)
    for c in range(ctx):
        mine += jnp.where(me_c == c, hidden[c * tok : (c + 1) * tok, :], 0.0)
    for copy in sends:
        copy.wait_send()
    finish(arrivals)
    routed = sum(fin_all[i].astype(F32) for i in range(grp * ctx * pairs))
    out_ref[...] = (mine + routed).astype(out_ref.dtype)


def fused_body(
    queries,
    latent_cache,
    cache_len,
    kv_up,
    o_weight,
    residual,
    norm_gain,
    route_ids,
    route_weights,
    w_gate,
    w_up,
    w_down,
):
    grp, ctx, sub = lax.axis_size("grp"), lax.axis_size("ctx"), lax.axis_size("sub")
    heads, tok, experts = kv_up.shape[0], queries.shape[0], w_gate.shape[0] // grp
    span, rows, quarter = ctx * tok, heads * ctx * tok, o_weight.shape[1]
    width, piece, everyone = residual.shape[1], quarter // sub, grp * ctx * sub
    w_gate, w_up = jnp.swapaxes(w_gate, 1, 2), jnp.swapaxes(w_up, 1, 2)
    units = experts * w_gate.shape[1]
    cache = latent_cache.T
    gain = norm_gain.reshape(width // LANES, LANES)
    hbm = pl.BlockSpec(memory_space=pl.ANY)
    dma = pltpu.SemaphoreType.DMA
    out = pl.pallas_call(
        functools.partial(fused_kernel, (grp, ctx, sub, tok, heads, experts)),
        out_shape=jax.ShapeDtypeStruct((tok, width // sub), F32),
        in_specs=[hbm] * 12,
        out_specs=pl.BlockSpec(memory_space=pltpu.VMEM),
        scratch_shapes=[
            pltpu.VMEM(residual.shape, BF16),
            pltpu.VMEM(route_ids.shape, jnp.int32),
            pltpu.VMEM(route_weights.shape, F32),
            pltpu.SMEM(cache_len.shape, jnp.int32),
            pltpu.VMEM(cache.shape, BF16),
            pltpu.VMEM(kv_up.shape, BF16),
            pltpu.VMEM(o_weight.shape, BF16),
            pltpu.VMEM(gain.shape, BF16),
            pltpu.VMEM((ctx,) + queries.shape, BF16),
            pltpu.VMEM((ctx, tok, piece), BF16),
            pltpu.VMEM((grp * ctx, tok, LANES), F32),
            pltpu.VMEM((grp * ctx, tok, LANES), F32),
            pltpu.VMEM((ctx, rows, LANES), BF16),
            pltpu.VMEM((ctx, rows, LANES), BF16),
            pltpu.VMEM((ctx, rows, LANES), BF16),
            pltpu.VMEM((ctx, CHUNKS, 8, rows // CHUNKS), F32),
            pltpu.VMEM((ctx, CHUNKS, span, heads * VDIM // CHUNKS), BF16),
            pltpu.VMEM((sub, span, piece), BF16),
            pltpu.VMEM((sub, span, piece), BF16),
            pltpu.VMEM((everyone, span, piece), BF16),
            pltpu.VMEM(gain.shape, F32),
            pltpu.VMEM((ctx, grp * span, quarter), BF16),
            pltpu.VMEM((grp * span, units), F32),
            pltpu.VMEM((grp * span, units), F32),
            pltpu.VMEM((grp * span, units), F32),
            pltpu.VMEM((grp * span, units), BF16),
            pltpu.VMEM((sub // 2, grp * span, quarter), BF16),
            pltpu.VMEM((sub // 2, grp * span, quarter), BF16),
            pltpu.VMEM((sub // 2, grp * span, quarter), F32),
            pltpu.VMEM((sub // 2, grp * ctx, tok, quarter), BF16),
            pltpu.VMEM((everyone // 2, tok, quarter), BF16),
            pltpu.VMEM((units, width), BF16),
            pltpu.VMEM((units, width), BF16),
            pltpu.VMEM((units, width), BF16),
            dma((9,)),
            dma((experts, 3)),
            dma((2 + 4 * CHUNKS, ctx)),
            dma((2 + 4 * CHUNKS, ctx)),
            dma((grp * ctx,)),
            dma((grp * ctx,)),
            dma((sub,)),
            dma((sub,)),
            dma((everyone,)),
            dma((everyone,)),
            dma((sub // 2,)),
            dma((sub // 2,)),
            dma((everyone // 2,)),
            dma((everyone // 2,)),
        ],
        compiler_params=pltpu.CompilerParams(
            collective_id=0, has_side_effects=True, vmem_limit_bytes=46 * 1024 * 1024
        ),
    )(
        *(
            operand
            if operand is cache_len
            else pltpu.with_memory_space_constraint(operand, pltpu.HBM)
            for operand in (
                queries,
                residual,
                route_ids,
                route_weights,
                cache_len,
                cache,
                kv_up,
                o_weight,
                gain,
                w_gate,
                w_up,
                w_down,
            )
        )
    )
    return out.astype(BF16)


def choose_body(*args):
    kv_up, o_weight, w_gate = args[3], args[4], args[9]
    grp, ctx, sub = lax.axis_size("grp"), lax.axis_size("ctx"), lax.axis_size("sub")
    tok, experts = args[0].shape[0], w_gate.shape[0]
    units = experts // grp * w_gate.shape[2]
    fits = (
        ctx == sub
        and ctx % 2 == 0
        and kv_up.shape[2] == LANES
        and o_weight.shape[1] == sub * LANES
        and kv_up.shape[0] * ctx * tok == LANES
        and experts % grp == 0
        and experts <= LANES
        and w_gate.shape[2] % 16 == 0
        and units % TILE == 0
        and o_weight.shape[1] % TILE == 0
        and units * w_gate.shape[1] * 6 <= 40 * 1024 * 1024
        and tok % 8 == 0
    )
    return fused_body(*args) if fits else body(*args)


def solution(mesh):
    in_specs = (
        P(("grp", "ctx"), "sub"),
        P(("grp", "ctx"), None),
        P(("grp", "ctx")),
        P(("grp", "sub"), None, "ctx"),
        P("sub", "ctx"),
        P(("grp", "ctx"), None),
        P(),
        P(("grp", "ctx"), None),
        P(("grp", "ctx"), None),
        P("ctx", None, "sub"),
        P("ctx", None, "sub"),
        P("ctx", "sub", None),
    )
    out_specs = P(("grp", "ctx"), "sub")
    return jax.shard_map(choose_body, mesh=mesh, in_specs=in_specs, out_specs=out_specs, check_vma=False)
```
